128 devices in a mesh: pool: 128 (over z, y, x, core).
Axes of the slice: x: 4, y: 4, z: 4, core: 2. Of those that a mesh axis runs over, the one named last changes fastest.
Arguments:
- queries: bfloat16 [128, 256, 32, 128], P('pool')
- k_new: bfloat16 [128, 256, 8, 128], P('pool')
- v_new: bfloat16 [128, 256, 8, 128], P('pool')
- k_pool: bfloat16 [4096, 16, 8, 128], P('pool')
- v_pool: bfloat16 [4096, 16, 8, 128], P('pool')
- block_table: int32 [128, 256], replicated
- write_ids: int32 [128, 16], P('pool')
Outputs:
- output 1: bfloat16 [128, 256, 32, 128], P('pool')
- output 2: bfloat16 [4096, 16, 8, 128], P('pool')
- output 3: bfloat16 [4096, 16, 8, 128], P('pool')
All inputs are finite; a program needn't handle non-finite values.
Results may differ from the reference program's by a relative error of at most 0.00944931.
Values are sent between devices in bfloat16 or wider.
A program may use at most 1 GiB of HBM per device.

```python
import jax
import jax.numpy as jnp
from jax import lax

NUM_DEVICES = 128
REQ_PER_DEV = 1
CHUNK_LEN = 256
PREFIX_BLOCKS = 256
BLOCKS_PER_DEV = 32
BLOCK_LEN = 16
Q_HEADS = 32
KV_HEADS = 8
HEAD_DIM = 128


def draw_tables(rng_key):
    key_first, key_choice, key_start, key_base, key_write = jax.random.split(rng_key, 5)
    quarter = BLOCKS_PER_DEV // 4
    half_len = PREFIX_BLOCKS // 2
    per_owner = 2 * PREFIX_BLOCKS // NUM_DEVICES
    first_dev = jax.random.randint(key_first, (), 0, NUM_DEVICES)
    dev_choice = jax.random.randint(key_choice, (NUM_DEVICES,), 0, 2)
    win_start = first_dev + jax.random.randint(key_start, (NUM_DEVICES,), 0, NUM_DEVICES // 4)
    row_base = jax.random.randint(key_base, (NUM_DEVICES, REQ_PER_DEV), 0, quarter)
    slot_idx = jnp.arange(half_len)
    pop_owner = (first_dev + slot_idx // per_owner) % NUM_DEVICES
    pop_local = dev_choice[:, None] * per_owner + slot_idx[None, :] % per_owner
    pop_ids = pop_owner[None, :] * BLOCKS_PER_DEV + pop_local
    pop_rows = jnp.broadcast_to(pop_ids[:, None, :], (NUM_DEVICES, REQ_PER_DEV, half_len))
    win_owner = (win_start[:, None] + slot_idx[None, :]) % NUM_DEVICES
    win_local = quarter + (row_base[:, :, None] + slot_idx[None, None, :] // NUM_DEVICES) % quarter
    win_rows = win_owner[:, None, :] * BLOCKS_PER_DEV + win_local
    block_tab = jnp.concatenate([pop_rows, win_rows], axis=-1)
    block_tab = block_tab.reshape(NUM_DEVICES * REQ_PER_DEV, PREFIX_BLOCKS)
    new_blocks = REQ_PER_DEV * CHUNK_LEN // BLOCK_LEN
    write_keys = jax.random.split(key_write, NUM_DEVICES)
    shuffled = jax.vmap(lambda one_key: jax.random.permutation(one_key, BLOCKS_PER_DEV // 2))(write_keys)
    write_tab = shuffled[:, :new_blocks] + BLOCKS_PER_DEV // 2
    write_tab = write_tab.reshape(NUM_DEVICES * REQ_PER_DEV, CHUNK_LEN // BLOCK_LEN)
    return block_tab.astype(jnp.int32), write_tab.astype(jnp.int32)


def setup_inputs(seed: int = 0) -> dict:
    key_q, key_kn, key_vn, key_kp, key_vp, key_tab = jax.random.split(jax.random.key(seed), 6)
    n_rows = NUM_DEVICES * REQ_PER_DEV
    chunk_kv = (n_rows, CHUNK_LEN, KV_HEADS, HEAD_DIM)
    pool_shape = (NUM_DEVICES * BLOCKS_PER_DEV, BLOCK_LEN, KV_HEADS, HEAD_DIM)
    queries = jax.random.normal(key_q, (n_rows, CHUNK_LEN, Q_HEADS, HEAD_DIM), jnp.float32)
    k_new = jax.random.normal(key_kn, chunk_kv, jnp.float32)
    v_new = jax.random.normal(key_vn, chunk_kv, jnp.float32)
    k_pool = jax.random.normal(key_kp, pool_shape, jnp.float32)
    v_pool = jax.random.normal(key_vp, pool_shape, jnp.float32)
    block_table, write_ids = draw_tables(key_tab)
    return {'queries': queries.astype(jnp.bfloat16), 'k_new': k_new.astype(jnp.bfloat16), 'v_new': v_new.astype(jnp.bfloat16), 'k_pool': k_pool.astype(jnp.bfloat16), 'v_pool': v_pool.astype(jnp.bfloat16), 'block_table': block_table, 'write_ids': write_ids}


def attend_one(q_rows, k_all, v_all):
    groups = Q_HEADS // KV_HEADS
    prefix_len = PREFIX_BLOCKS * BLOCK_LEN
    q_grp = q_rows.astype(jnp.float32).reshape(CHUNK_LEN, KV_HEADS, groups, HEAD_DIM)
    scores = jnp.einsum('cgqd,tgd->cgqt', q_grp, k_all.astype(jnp.float32)) * HEAD_DIM ** -0.5
    visible = jnp.arange(prefix_len + CHUNK_LEN)[None, :] <= prefix_len + jnp.arange(CHUNK_LEN)[:, None]
    scores = jnp.where(visible[:, None, None, :], scores, -jnp.inf)
    prob_rows = jax.nn.softmax(scores, axis=-1).astype(jnp.bfloat16).astype(jnp.float32)
    attn_rows = jnp.einsum('cgqt,tgd->cgqd', prob_rows, v_all.astype(jnp.float32))
    return attn_rows.reshape(CHUNK_LEN, Q_HEADS, HEAD_DIM).astype(jnp.bfloat16)


def reference(queries, k_new, v_new, k_pool, v_pool, block_table, write_ids):
    prefix_len = PREFIX_BLOCKS * BLOCK_LEN
    n_rows = NUM_DEVICES * REQ_PER_DEV

    def one_request(row_item):
        q_rows, k_chunk, v_chunk, row_ids = row_item
        k_all = jnp.concatenate([k_pool[row_ids].reshape(prefix_len, KV_HEADS, HEAD_DIM), k_chunk], axis=0)
        v_all = jnp.concatenate([v_pool[row_ids].reshape(prefix_len, KV_HEADS, HEAD_DIM), v_chunk], axis=0)
        return attend_one(q_rows, k_all, v_all)

    attn_out = lax.map(one_request, (queries, k_new, v_new, block_table))
    targets = ((jnp.arange(n_rows) // REQ_PER_DEV)[:, None] * BLOCKS_PER_DEV + write_ids).reshape(-1)
    new_shape = (n_rows * CHUNK_LEN // BLOCK_LEN, BLOCK_LEN, KV_HEADS, HEAD_DIM)
    k_pool_out = k_pool.at[targets].set(k_new.reshape(new_shape))
    v_pool_out = v_pool.at[targets].set(v_new.reshape(new_shape))
    return attn_out, k_pool_out, v_pool_out
```

```python
import functools

import jax
import jax.numpy as jnp
from jax import lax
from jax.experimental import pallas as pl
from jax.experimental.pallas import tpu as pltpu
from jax.sharding import PartitionSpec as P


def peer_of(me, offset):
    z = ((me // 32) + (offset // 32)) % 4
    y = ((me // 8) % 4 + (offset // 8) % 4) % 4
    x = ((me // 2) % 4 + (offset // 2) % 4) % 4
    c = (me % 2 + offset % 2) % 2
    return z * 32 + y * 8 + x * 2 + c


def exchange_kernel(n_dev, src_ref, dst_ref, send_sem, recv_sem, self_sem):
    me = lax.axis_index('pool')
    barrier = pltpu.get_barrier_semaphore()

    def greet(i, carry):
        pl.semaphore_signal(barrier, inc=1, device_id=(peer_of(me, i),), device_id_type=pl.DeviceIdType.MESH)
        return carry

    lax.fori_loop(1, n_dev, greet, 0)
    pl.semaphore_wait(barrier, n_dev - 1)
    own = pltpu.make_async_copy(src_ref.at[me], dst_ref.at[me], self_sem)
    own.start()

    def copy_to(i):
        peer = peer_of(me, (i * 37) % n_dev)
        return pltpu.make_async_remote_copy(
            src_ref=src_ref.at[peer], dst_ref=dst_ref.at[me], send_sem=send_sem, recv_sem=recv_sem,
            device_id=(peer,), device_id_type=pl.DeviceIdType.MESH)

    def send(i, carry):
        copy_to(i).start()
        return carry

    lax.fori_loop(1, n_dev, send, 0)
    rest = pltpu.make_async_remote_copy(
        src_ref=src_ref.at[pl.ds(0, n_dev - 1)], dst_ref=dst_ref.at[pl.ds(0, n_dev - 1)], send_sem=send_sem,
        recv_sem=recv_sem, device_id=(peer_of(me, 1),), device_id_type=pl.DeviceIdType.MESH)
    rest.wait_send()
    rest.wait_recv()
    own.wait()


def exchange(blocks, collective_id):
    n_dev = blocks.shape[0]
    return pl.pallas_call(
        functools.partial(exchange_kernel, n_dev),
        out_shape=jax.ShapeDtypeStruct(blocks.shape, blocks.dtype),
        in_specs=[pl.BlockSpec(memory_space=pl.ANY)],
        out_specs=pl.BlockSpec(memory_space=pl.ANY),
        scratch_shapes=[pltpu.SemaphoreType.DMA, pltpu.SemaphoreType.DMA, pltpu.SemaphoreType.DMA],
        compiler_params=pltpu.CompilerParams(has_side_effects=True, collective_id=collective_id),
        name='block_exchange')(blocks)


def chunk_attention(q_grp, k_pref, v_pref, k_chunk, v_chunk):
    chunk_len = q_grp.shape[1]
    score_scale = q_grp.shape[-1] ** -0.5
    s_pref = jnp.einsum('rcgqd,rtgd->rcgqt', q_grp, k_pref, preferred_element_type=jnp.float32) * score_scale
    s_self = jnp.einsum('rcgqd,rtgd->rcgqt', q_grp, k_chunk, preferred_element_type=jnp.float32) * score_scale
    causal = (jnp.arange(chunk_len)[:, None] >= jnp.arange(chunk_len)[None, :])[None, :, None, None, :]
    s_self = jnp.where(causal, s_self, -jnp.inf)
    row_max = jnp.maximum(jnp.max(s_pref, axis=-1), jnp.max(s_self, axis=-1))[..., None]
    e_pref = jnp.exp(s_pref - row_max)
    e_self = jnp.exp(s_self - row_max)
    prob_total = jnp.sum(e_pref, axis=-1, keepdims=True) + jnp.sum(e_self, axis=-1, keepdims=True)
    p_pref = (e_pref / prob_total).astype(jnp.bfloat16)
    p_self = (e_self / prob_total).astype(jnp.bfloat16)
    attn_acc = jnp.einsum('rcgqt,rtgd->rcgqd', p_pref, v_pref, preferred_element_type=jnp.float32)
    return attn_acc + jnp.einsum('rcgqt,rtgd->rcgqd', p_self, v_chunk, preferred_element_type=jnp.float32)


def solution(mesh):
    n_dev = mesh.shape['pool']

    def local_step(queries, k_new, v_new, k_pool, v_pool, block_table, write_ids):
        req_count, chunk_len, q_heads, head_dim = queries.shape
        kv_heads = k_new.shape[2]
        per_dev, block_len = k_pool.shape[0], k_pool.shape[1]
        n_pref = block_table.shape[1]
        row_cap = 2 * n_pref // n_dev + (n_pref // 2 + n_dev - 1) // n_dev
        pair_cap = req_count * row_cap
        my_index = lax.axis_index('pool')
        owners = block_table // per_dev
        owned_here = (owners == my_index).reshape(n_dev, req_count * n_pref).astype(jnp.int32)
        send_slot = jnp.where(owned_here > 0, jnp.cumsum(owned_here, axis=1) - 1, pair_cap)
        dest_dev = jnp.broadcast_to(jnp.arange(n_dev)[:, None], send_slot.shape)
        local_ids = (block_table % per_dev).reshape(n_dev, req_count * n_pref)
        send_ids = jnp.zeros((n_dev, pair_cap), jnp.int32).at[dest_dev, send_slot].set(local_ids, mode='drop')
        k_recv = exchange(k_pool[send_ids], 0)
        v_recv = exchange(v_pool[send_ids], 0)
        my_owners = lax.dynamic_slice_in_dim(owners, my_index * req_count, req_count, 0).reshape(-1)
        from_owner = (my_owners[:, None] == jnp.arange(n_dev)[None, :]).astype(jnp.int32)
        slot_rank = jnp.sum(from_owner * (jnp.cumsum(from_owner, axis=0) - 1), axis=1)
        recv_idx = (my_owners * pair_cap + slot_rank).reshape(req_count, n_pref)
        flat_shape = (n_dev * pair_cap, block_len, kv_heads, head_dim)
        prefix_shape = (req_count, n_pref * block_len, kv_heads, head_dim)
        k_pref = k_recv.reshape(flat_shape)[recv_idx].reshape(prefix_shape)
        v_pref = v_recv.reshape(flat_shape)[recv_idx].reshape(prefix_shape)
        q_grp = queries.reshape(req_count, chunk_len, kv_heads, q_heads // kv_heads, head_dim)
        attn_acc = chunk_attention(q_grp, k_pref, v_pref, k_new, v_new)
        attn_out = attn_acc.reshape(req_count, chunk_len, q_heads, head_dim).astype(jnp.bfloat16)
        new_shape = (req_count * chunk_len // block_len, block_len, kv_heads, head_dim)
        targets = write_ids.reshape(-1)
        k_pool_out = k_pool.at[targets].set(k_new.reshape(new_shape))
        v_pool_out = v_pool.at[targets].set(v_new.reshape(new_shape))
        return attn_out, k_pool_out, v_pool_out

    row_spec = P('pool')
    return jax.shard_map(local_step, mesh=mesh, in_specs=(row_spec, row_spec, row_spec, row_spec, row_spec, P(), row_spec), out_specs=(row_spec, row_spec, row_spec), check_vma=False)
```

```python
import functools
import math

import jax
import jax.numpy as jnp
from jax import lax
from jax.experimental import pallas as pl
from jax.experimental.pallas import tpu as pltpu
from jax.sharding import PartitionSpec as P

COMMON = 8
GROUP = 32
MESH = pl.DeviceIdType.MESH


def chunk_attention(q_grp, k_pref, v_pref, k_chunk, v_chunk):
    chunk_len = q_grp.shape[1]
    score_scale = q_grp.shape[-1] ** -0.5
    s_pref = jnp.einsum('rcgqd,rtgd->rcgqt', q_grp, k_pref, preferred_element_type=jnp.float32) * score_scale
    s_self = jnp.einsum('rcgqd,rtgd->rcgqt', q_grp, k_chunk, preferred_element_type=jnp.float32) * score_scale
    causal = (jnp.arange(chunk_len)[:, None] >= jnp.arange(chunk_len)[None, :])[None, :, None, None, :]
    s_self = jnp.where(causal, s_self, -jnp.inf)
    row_max = jnp.maximum(jnp.max(s_pref, axis=-1), jnp.max(s_self, axis=-1))[..., None]
    e_pref = jnp.exp(s_pref - row_max)
    e_self = jnp.exp(s_self - row_max)
    prob_total = jnp.sum(e_pref, axis=-1, keepdims=True) + jnp.sum(e_self, axis=-1, keepdims=True)
    p_pref = (e_pref / prob_total).astype(jnp.bfloat16)
    p_self = (e_self / prob_total).astype(jnp.bfloat16)
    attn_acc = jnp.einsum('rcgqt,rtgd->rcgqd', p_pref, v_pref, preferred_element_type=jnp.float32)
    return attn_acc + jnp.einsum('rcgqt,rtgd->rcgqd', p_self, v_chunk, preferred_element_type=jnp.float32)


def general_attention(n_dev, queries, k_new, v_new, k_pool, v_pool, block_table):
    req_count, chunk_len, q_heads, head_dim = queries.shape
    kv_heads = k_new.shape[2]
    per_dev, block_len = k_pool.shape[0], k_pool.shape[1]
    n_pref = block_table.shape[1]
    row_cap = 2 * n_pref // n_dev + (n_pref // 2 + n_dev - 1) // n_dev
    pair_cap = req_count * row_cap
    my_index = lax.axis_index('pool')
    owners = block_table // per_dev
    owned_here = (owners == my_index).reshape(n_dev, req_count * n_pref).astype(jnp.int32)
    send_slot = jnp.where(owned_here > 0, jnp.cumsum(owned_here, axis=1) - 1, pair_cap)
    dest_dev = jnp.broadcast_to(jnp.arange(n_dev)[:, None], send_slot.shape)
    local_ids = (block_table % per_dev).reshape(n_dev, req_count * n_pref)
    send_ids = jnp.zeros((n_dev, pair_cap), jnp.int32).at[dest_dev, send_slot].set(local_ids, mode='drop')
    k_recv = lax.all_to_all(k_pool[send_ids], 'pool', 0, 0, tiled=True)
    v_recv = lax.all_to_all(v_pool[send_ids], 'pool', 0, 0, tiled=True)
    my_owners = lax.dynamic_slice_in_dim(owners, my_index * req_count, req_count, 0).reshape(-1)
    from_owner = (my_owners[:, None] == jnp.arange(n_dev)[None, :]).astype(jnp.int32)
    slot_rank = jnp.sum(from_owner * (jnp.cumsum(from_owner, axis=0) - 1), axis=1)
    recv_idx = (my_owners * pair_cap + slot_rank).reshape(req_count, n_pref)
    flat_shape = (n_dev * pair_cap, block_len, kv_heads, head_dim)
    prefix_shape = (req_count, n_pref * block_len, kv_heads, head_dim)
    k_pref = k_recv.reshape(flat_shape)[recv_idx].reshape(prefix_shape)
    v_pref = v_recv.reshape(flat_shape)[recv_idx].reshape(prefix_shape)
    q_grp = queries.reshape(req_count, chunk_len, kv_heads, q_heads // kv_heads, head_dim)
    attn_acc = chunk_attention(q_grp, k_pref, v_pref, k_new, v_new)
    return attn_acc.reshape(req_count, chunk_len, q_heads, head_dim).astype(jnp.bfloat16)


def plan_exchange(block_table, per_dev, n_dev):
    me = lax.axis_index('pool')
    n_col = n_dev // 4
    owners, locals_ = block_table // per_dev, block_table % per_dev
    owner_hot = (owners[:, :, None] == jnp.arange(n_dev)).astype(jnp.bfloat16)
    local_hot = (locals_[:, :, None] == jnp.arange(per_dev)).astype(jnp.bfloat16)
    named = jnp.einsum('ril,rio->rlo', local_hot, owner_hot, preferred_element_type=jnp.float32) > 0
    use_count = jnp.sum(named.astype(jnp.int32), axis=0)
    local_id = jnp.arange(per_dev, dtype=jnp.int32)[:, None]
    none = jnp.int32(1 << 20)
    key = jnp.where(named, (use_count * per_dev + local_id)[None], none)
    least = jnp.min(key, axis=1)
    common_use = named & (key > least[:, None, :])
    common = jnp.any(common_use, axis=0)
    earlier = (local_id > local_id.T).astype(jnp.bfloat16)
    rank = jnp.dot(earlier, common.astype(jnp.bfloat16), preferred_element_type=jnp.float32).astype(jnp.int32)
    per_owner = jnp.sum(common.astype(jnp.int32), axis=0).reshape(4, n_col)
    base = jnp.cumsum(per_owner, axis=0) - per_owner
    fits = jnp.all(least < none) & jnp.all(jnp.sum(per_owner, axis=0) <= COMMON)
    in_col = base.reshape(1, n_dev) + rank
    column = jnp.arange(n_dev, dtype=jnp.int32) % n_col
    slot = column[None, :] * COMMON + in_col
    direct_ids = lax.dynamic_index_in_dim(least, me, 1, keepdims=False) % per_dev
    my_common = lax.dynamic_index_in_dim(common, me, 1, keepdims=False)
    my_rank = lax.dynamic_index_in_dim(rank, me, 1, keepdims=False)
    steps = jnp.arange(COMMON, dtype=jnp.int32)
    own_ids = jnp.sum(jnp.where(my_common[:, None] & (my_rank[:, None] == steps), local_id, 0), axis=0)
    source = (jnp.arange(n_dev, dtype=jnp.int32) // n_col)[None, :] * COMMON + rank
    here = common & (column == me % n_col)[None, :]
    col_ids = jnp.sum(jnp.where(here[:, :, None] & (in_col[:, :, None] == steps), source[:, :, None], 0), axis=(0, 1))
    mine = (lax.dynamic_index_in_dim(named, me, 0, keepdims=False) & common).T.reshape(-1)
    place = jnp.cumsum(mine.astype(jnp.int32).reshape(n_dev, per_dev), axis=1)
    before = jnp.cumsum(place[:, -1]) - place[:, -1]
    place = (place - 1 + before[:, None]).reshape(-1)
    picks = jnp.arange(n_dev, dtype=jnp.int32)
    pick_ids = jnp.sum(jnp.where(mine[:, None] & (place[:, None] == picks), slot.T.reshape(-1, 1), 0), axis=0)
    return fits, direct_ids, own_ids, col_ids, pick_ids


def device_at(z, y, x, c):
    return z * 32 + y * 8 + x * 2 + c


def fused_kernel(direct_ref, own_ref, col_ref, pick_ref, q_ref, kn_ref, vn_ref, kv_ref, o_ref,
                 zbuf, cbuf, sbuf, wbuf, pbuf, acc_ref, m_ref, l_ref,
                 z_send, z_recv, a_send, a_recv, b_send, b_recv, c_send, c_recv, w_send, w_recv):
    n_dev, kv_heads = 128, kn_ref.shape[0]
    q_rows = q_ref.shape[1]
    heads = 4
    q_tile = q_rows // heads
    scale = math.log2(math.e) * q_ref.shape[2] ** -0.5
    me = lax.axis_index('pool')
    z, y, x, c = me // 32, (me // 8) % 4, (me // 2) % 4, me % 2
    col = me % 32

    def offset_peer(i):
        o = (i * 37) % n_dev
        return device_at((z + o // 32) % 4, (y + (o // 8) % 4) % 4, (x + (o // 2) % 4) % 4, (c + o) % 2)

    barrier = pltpu.get_barrier_semaphore()

    def greet(i, carry):
        pl.semaphore_signal(barrier, inc=1, device_id=(offset_peer(i),), device_id_type=MESH)
        return carry

    lax.fori_loop(1, n_dev, greet, 0)

    for k in range(COMMON):
        zbuf[z * COMMON + k] = kv_ref[own_ref[k]]

    def fill(i, carry):
        sbuf[i] = kv_ref[direct_ref[offset_peer(i)]]
        return carry

    lax.fori_loop(1, n_dev, fill, 0)
    wbuf[0] = kv_ref[direct_ref[me]]
    pl.semaphore_wait(barrier, n_dev - 1)

    def remote(src, dst, ssem, rsem, peer):
        return pltpu.make_async_remote_copy(src_ref=src, dst_ref=dst, send_sem=ssem, recv_sem=rsem,
                                            device_id=(peer,), device_id_type=MESH)

    z_part = zbuf.at[pl.ds(z * COMMON, COMMON)]
    for s in range(1, 4):
        remote(z_part, z_part, z_send, z_recv, device_at((z + s) % 4, y, x, c)).start()

    def send_direct(group):
        def one(i, carry):
            remote(sbuf.at[i], wbuf.at[i], w_send.at[group], w_recv.at[group], offset_peer(i)).start()
            return carry
        lax.fori_loop(max(1, group * GROUP), (group + 1) * GROUP, one, 0)

    other = device_at(z, y, x, 1 - c)

    def wait_direct(group):
        size = GROUP - 1 if group == 0 else GROUP
        part = wbuf.at[pl.ds(0, size)]
        remote(part, part, w_send.at[group], w_recv.at[group], other).wait_recv()

    def attend(keys, values, first):
        def per_head(g, carry):
            k_g, v_g = keys(g), values(g)
            for h in range(heads):
                cols = pl.ds(h * q_tile, q_tile)
                s = lax.dot_general(k_g, q_ref[g, cols, :], (((1,), (1,)), ((), ())), preferred_element_type=jnp.float32)
                if first:
                    row = lax.broadcasted_iota(jnp.int32, s.shape, 0)
                    token = lax.broadcasted_iota(jnp.int32, s.shape, 1)
                    s = jnp.where(row <= token, s, -jnp.inf)
                top = jnp.max(s, axis=0, keepdims=True)
                if not first:
                    old = m_ref[g, :, cols]
                    top = jnp.maximum(top, old)
                    fade = jnp.exp2((old - top) * scale)
                e = jnp.exp2((s - top) * scale)
                total = jnp.sum(e, axis=0, keepdims=True)
                part = lax.dot_general(v_g, e.astype(jnp.bfloat16), (((0,), (0,)), ((), ())), preferred_element_type=jnp.float32)
                m_ref[g, :, cols] = top
                if first:
                    l_ref[g, :, cols] = total
                    acc_ref[g, :, cols] = part
                else:
                    l_ref[g, :, cols] = l_ref[g, :, cols] * fade + total
                    acc_ref[g, :, cols] = acc_ref[g, :, cols] * fade + part
            return carry
        lax.fori_loop(0, kv_heads, per_head, 0)

    def attend_blocks(ref, start):
        def side(which):
            def of(g):
                rows = ref[pl.ds(start, GROUP), which, g]
                return rows.reshape(GROUP * rows.shape[1], rows.shape[2])
            return of
        attend(side(0), side(1), False)

    send_direct(0)
    attend(lambda g: kn_ref[g], lambda g: vn_ref[g], True)

    remote(zbuf.at[pl.ds(0, 3 * COMMON)], zbuf.at[pl.ds(0, 3 * COMMON)], z_send, z_recv, other).wait_recv()
    for k in range(COMMON):
        cbuf[col * COMMON + k] = zbuf[col_ref[k]]
    y_first = (c == 0).astype(jnp.int32)

    def peer_a(s):
        return device_at(z, (y + s * y_first) % 4, (x + s * (1 - y_first)) % 4, c)

    def peer_b(s):
        return device_at(z, (y + s * (1 - y_first)) % 4, (x + s * y_first) % 4, c)

    def line_column(yy, xx):
        return (yy % 4) * 8 + (xx % 4) * 2 + c

    def part_of(column):
        return cbuf.at[pl.ds(column * COMMON, COMMON)]

    own_part = part_of(col)
    for s in range(1, 4):
        remote(own_part, own_part, a_send, a_recv, peer_a(s)).start()
    remote(own_part, own_part, c_send.at[0], c_recv.at[0], other).start()
    send_direct(1)
    wait_direct(0)
    attend_blocks(wbuf, 0)
    three = cbuf.at[pl.ds(0, 3 * COMMON)]
    four = cbuf.at[pl.ds(0, 4 * COMMON)]
    remote(three, three, a_send, a_recv, other).wait_recv()
    lines = [part_of(line_column(y + i * y_first, x + i * (1 - y_first))) for i in range(4)]
    for s in range(1, 4):
        for line in lines:
            remote(line, line, b_send, b_recv.at[s - 1], peer_b(s)).start()
    for line in lines[1:]:
        remote(line, line, c_send.at[0], c_recv.at[0], other).start()
    send_direct(2)
    wait_direct(1)
    attend_blocks(wbuf, GROUP)
    send_direct(3)
    for s in range(1, 4):
        remote(four, four, b_send, b_recv.at[s - 1], other).wait_recv()
        for i in range(4):
            line = part_of(line_column(y + i * y_first - s * (1 - y_first), x + i * (1 - y_first) - s * y_first))
            remote(line, line, c_send.at[s], c_recv.at[s], other).start()
    wait_direct(2)
    attend_blocks(wbuf, 2 * GROUP)
    for s in range(4):
        remote(four, four, c_send.at[s], c_recv.at[s], other).wait_recv()

    def attend_common(group, carry):
        def pick(i, inner):
            pbuf[i] = cbuf[pick_ref[group * GROUP + i]]
            return inner
        lax.fori_loop(0, GROUP, pick, 0)
        attend_blocks(pbuf, 0)
        return carry

    lax.fori_loop(0, n_dev // GROUP, attend_common, 0)
    wait_direct(3)
    attend_blocks(wbuf, 3 * GROUP)

    def finish(g, carry):
        for h in range(heads):
            cols = pl.ds(h * q_tile, q_tile)
            out = acc_ref[g, :, cols] / l_ref[g, :, cols]
            o_ref[g, cols, :] = out.T.astype(jnp.bfloat16)
        return carry

    lax.fori_loop(0, kv_heads, finish, 0)

    remote(zbuf.at[pl.ds(0, 3 * COMMON)], zbuf.at[pl.ds(0, 3 * COMMON)], z_send, z_recv, other).wait_send()
    remote(three, three, a_send, a_recv, other).wait_send()
    twelve = cbuf.at[pl.ds(0, 12 * COMMON)]
    remote(twelve, twelve, b_send, b_recv.at[0], other).wait_send()
    for s in range(4):
        remote(four, four, c_send.at[s], c_recv.at[s], other).wait_send()
    for group in range(4):
        size = GROUP - 1 if group == 0 else GROUP
        part = wbuf.at[pl.ds(0, size)]
        remote(part, part, w_send.at[group], w_recv.at[group], other).wait_send()


def fused_attention(queries, k_new, v_new, kv, direct_ids, own_ids, col_ids, pick_ids):
    _, chunk_len, q_heads, head_dim = queries.shape
    kv_heads = k_new.shape[2]
    q_grp = queries[0].transpose(1, 0, 2).reshape(kv_heads, -1, head_dim)
    k_own, v_own = k_new[0].transpose(1, 0, 2), v_new[0].transpose(1, 0, 2)
    block = kv.shape[1:]
    bf16, f32 = jnp.bfloat16, jnp.float32
    smem, vmem = pl.BlockSpec(memory_space=pltpu.SMEM), pl.BlockSpec(memory_space=pltpu.VMEM)
    dma = pltpu.SemaphoreType.DMA
    out = pl.pallas_call(
        fused_kernel,
        out_shape=jax.ShapeDtypeStruct(q_grp.shape, bf16),
        in_specs=[smem] * 4 + [vmem] * 4,
        out_specs=vmem,
        scratch_shapes=[
            pltpu.VMEM((4 * COMMON,) + block, bf16),
            pltpu.VMEM((32 * COMMON,) + block, bf16),
            pltpu.VMEM((128,) + block, bf16),
            pltpu.VMEM((128,) + block, bf16),
            pltpu.VMEM((GROUP,) + block, bf16),
            pltpu.VMEM((kv_heads, head_dim, q_grp.shape[1]), f32),
            pltpu.VMEM((kv_heads, 1, q_grp.shape[1]), f32),
            pltpu.VMEM((kv_heads, 1, q_grp.shape[1]), f32),
            dma, dma, dma, dma, dma, dma((3,)), dma((4,)), dma((4,)), dma((4,)), dma((4,)),
        ],
        compiler_params=pltpu.CompilerParams(has_side_effects=True, collective_id=0, vmem_limit_bytes=66_000_000),
        name='fused_attention')(direct_ids, own_ids, col_ids, pick_ids, q_grp, k_own, v_own, kv)
    return out.reshape(q_heads, chunk_len, head_dim).transpose(1, 0, 2)[None]


def solution(mesh):
    n_dev = mesh.shape['pool']

    def local_step(queries, k_new, v_new, k_pool, v_pool, block_table, write_ids):
        req_count, chunk_len, q_heads, head_dim = queries.shape
        kv_heads = k_new.shape[2]
        per_dev, block_len = k_pool.shape[0], k_pool.shape[1]
        fits, direct_ids, own_ids, col_ids, pick_ids = plan_exchange(block_table, per_dev, n_dev)
        kv = jnp.stack([k_pool.transpose(0, 2, 1, 3), v_pool.transpose(0, 2, 1, 3)], axis=1)
        attn_out = lax.cond(
            fits,
            lambda: fused_attention(queries, k_new, v_new, kv, direct_ids, own_ids, col_ids, pick_ids),
            lambda: general_attention(n_dev, queries, k_new, v_new, k_pool, v_pool, block_table))
        new_shape = (req_count * chunk_len // block_len, block_len, kv_heads, head_dim)
        targets = write_ids.reshape(-1)
        k_pool_out = k_pool.at[targets].set(k_new.reshape(new_shape))
        v_pool_out = v_pool.at[targets].set(v_new.reshape(new_shape))
        return attn_out, k_pool_out, v_pool_out

    row_spec = P('pool')
    return jax.shard_map(local_step, mesh=mesh, in_specs=(row_spec, row_spec, row_spec, row_spec, row_spec, P(), row_spec), out_specs=(row_spec, row_spec, row_spec), check_vma=False)
```

```python
import functools
import math

import jax
import jax.numpy as jnp
from jax import lax
from jax.experimental import pallas as pl
from jax.experimental.pallas import tpu as pltpu
from jax.sharding import PartitionSpec as P

COMMON = 8
GROUP = 32
MESH = pl.DeviceIdType.MESH


def chunk_attention(q_grp, k_pref, v_pref, k_chunk, v_chunk):
    chunk_len = q_grp.shape[1]
    score_scale = q_grp.shape[-1] ** -0.5
    s_pref = jnp.einsum('rcgqd,rtgd->rcgqt', q_grp, k_pref, preferred_element_type=jnp.float32) * score_scale
    s_self = jnp.einsum('rcgqd,rtgd->rcgqt', q_grp, k_chunk, preferred_element_type=jnp.float32) * score_scale
    causal = (jnp.arange(chunk_len)[:, None] >= jnp.arange(chunk_len)[None, :])[None, :, None, None, :]
    s_self = jnp.where(causal, s_self, -jnp.inf)
    row_max = jnp.maximum(jnp.max(s_pref, axis=-1), jnp.max(s_self, axis=-1))[..., None]
    e_pref = jnp.exp(s_pref - row_max)
    e_self = jnp.exp(s_self - row_max)
    prob_total = jnp.sum(e_pref, axis=-1, keepdims=True) + jnp.sum(e_self, axis=-1, keepdims=True)
    p_pref = (e_pref / prob_total).astype(jnp.bfloat16)
    p_self = (e_self / prob_total).astype(jnp.bfloat16)
    attn_acc = jnp.einsum('rcgqt,rtgd->rcgqd', p_pref, v_pref, preferred_element_type=jnp.float32)
    return attn_acc + jnp.einsum('rcgqt,rtgd->rcgqd', p_self, v_chunk, preferred_element_type=jnp.float32)


def general_attention(n_dev, queries, k_new, v_new, k_pool, v_pool, block_table):
    req_count, chunk_len, q_heads, head_dim = queries.shape
    kv_heads = k_new.shape[2]
    per_dev, block_len = k_pool.shape[0], k_pool.shape[1]
    n_pref = block_table.shape[1]
    row_cap = 2 * n_pref // n_dev + (n_pref // 2 + n_dev - 1) // n_dev
    pair_cap = req_count * row_cap
    my_index = lax.axis_index('pool')
    owners = block_table // per_dev
    owned_here = (owners == my_index).reshape(n_dev, req_count * n_pref).astype(jnp.int32)
    send_slot = jnp.where(owned_here > 0, jnp.cumsum(owned_here, axis=1) - 1, pair_cap)
    dest_dev = jnp.broadcast_to(jnp.arange(n_dev)[:, None], send_slot.shape)
    local_ids = (block_table % per_dev).reshape(n_dev, req_count * n_pref)
    send_ids = jnp.zeros((n_dev, pair_cap), jnp.int32).at[dest_dev, send_slot].set(local_ids, mode='drop')
    k_recv = lax.all_to_all(k_pool[send_ids], 'pool', 0, 0, tiled=True)
    v_recv = lax.all_to_all(v_pool[send_ids], 'pool', 0, 0, tiled=True)
    my_owners = lax.dynamic_slice_in_dim(owners, my_index * req_count, req_count, 0).reshape(-1)
    from_owner = (my_owners[:, None] == jnp.arange(n_dev)[None, :]).astype(jnp.int32)
    slot_rank = jnp.sum(from_owner * (jnp.cumsum(from_owner, axis=0) - 1), axis=1)
    recv_idx = (my_owners * pair_cap + slot_rank).reshape(req_count, n_pref)
    flat_shape = (n_dev * pair_cap, block_len, kv_heads, head_dim)
    prefix_shape = (req_count, n_pref * block_len, kv_heads, head_dim)
    k_pref = k_recv.reshape(flat_shape)[recv_idx].reshape(prefix_shape)
    v_pref = v_recv.reshape(flat_shape)[recv_idx].reshape(prefix_shape)
    q_grp = queries.reshape(req_count, chunk_len, kv_heads, q_heads // kv_heads, head_dim)
    attn_acc = chunk_attention(q_grp, k_pref, v_pref, k_new, v_new)
    return attn_acc.reshape(req_count, chunk_len, q_heads, head_dim).astype(jnp.bfloat16)


NT = (((1,), (1,)), ((), ()))
TN = (((0,), (0,)), ((), ()))


def plan_kernel(tab_ref, plan_ref, named_ref, least_ref):
    f32, bf16, i32 = jnp.float32, jnp.bfloat16, jnp.int32
    n_dev, n_pref = tab_ref.shape
    per_dev, n_col = 32, n_dev // 4
    me = lax.axis_index('pool')
    none = 1e6

    def iota(shape, dim):
        return lax.broadcasted_iota(i32, shape, dim)

    def ones(mask):
        return jnp.where(mask, 1.0, 0.0).astype(f32)

    def dot(a, b, dims=(((1,), (0,)), ((), ()))):
        return lax.dot_general(a.astype(bf16), b.astype(bf16), dims, preferred_element_type=f32)

    local_row = iota((per_dev, n_pref), 0)
    owner_row = iota((n_dev, n_pref), 0)
    local = iota((per_dev, n_dev), 0)
    owner = iota((per_dev, n_dev), 1)

    def count_row(r, total):
        row = tab_ref[pl.ds(r, 1), :]
        named = dot(ones(local_row == row % per_dev), ones(owner_row == row // per_dev), NT)
        named_ref[r] = named
        return total + named

    use_count = lax.fori_loop(0, n_dev, count_row, jnp.zeros((per_dev, n_dev), f32), unroll=8)
    order = use_count * per_dev + local.astype(f32)

    def split_row(r, carry):
        common, worst = carry
        named = named_ref[r] > 0
        key = jnp.where(named, order, none)
        least = jnp.min(key, axis=0, keepdims=True)
        least_ref[pl.ds(r, 1), :] = least
        common = jnp.maximum(common, ones(named & (key > least)))
        return common, jnp.maximum(worst, least)

    common, worst = lax.fori_loop(0, n_dev, split_row, (jnp.zeros((per_dev, n_dev), f32), jnp.zeros((1, n_dev), f32)), unroll=8)
    tri = ones(iota((per_dev, per_dev), 0) > iota((per_dev, per_dev), 1))
    rank = dot(tri, common)
    one_row = jnp.ones((8, per_dev), f32)
    source, target = iota((n_dev, n_dev), 0), iota((n_dev, n_dev), 1)
    per_owner = dot(one_row, common)
    same_col = source % n_col == target % n_col
    base = dot(per_owner, ones(same_col & (source < target)))[:1]
    in_all = dot(per_owner, ones(same_col))[:1]
    misfit = jnp.maximum(jnp.max(ones(worst >= none)), jnp.max(ones(in_all > COMMON)))
    in_col = base + rank
    slot = (owner % n_col * COMMON).astype(f32) + in_col
    pick_me = ones(iota((8, n_dev), 1) == me)
    direct = dot(pick_me, (least_ref[...].astype(i32) % per_dev).astype(f32), NT)[:1]
    here = owner == me
    my_common = jnp.sum(jnp.where(here, common, 0.0), axis=1, keepdims=True)
    my_rank = jnp.sum(jnp.where(here, rank, 0.0), axis=1, keepdims=True)
    lane = owner.astype(f32)
    own = jnp.sum(jnp.where((my_common > 0) & (my_rank == lane), local.astype(f32), 0.0), axis=0, keepdims=True)
    in_my_col = (common > 0) & (owner % n_col == me % n_col)
    place_in_z = (owner // n_col * COMMON).astype(f32) + rank
    lane_row = iota((1, n_dev), 1)
    col = jnp.zeros((1, n_dev), f32)
    for k in range(COMMON):
        found = jnp.sum(jnp.where(in_my_col & (in_col == k), place_in_z, 0.0))
        col = jnp.where(lane_row == k, found, col)
    mine = named_ref[me] * common
    before = dot(dot(one_row, mine), ones(source < target))[:1]
    place = jnp.where(mine > 0, dot(tri, mine) + before, -1.0).T
    slot_t = slot.T
    j_lane = target.astype(f32)
    pick = jnp.zeros((n_dev, n_dev), f32)
    for l in range(per_dev):
        pick = pick + jnp.where(place[:, l:l + 1] == j_lane, slot_t[:, l:l + 1], 0.0)
    pick = jnp.sum(pick, axis=0, keepdims=True)
    plan_ref[...] = jnp.zeros(plan_ref.shape, i32)
    for i, value in enumerate((misfit + jnp.zeros((1, n_dev), f32), direct, own, col, pick)):
        plan_ref[i:i + 1, :] = value.astype(i32)


def plan_exchange(block_table):
    n_dev = block_table.shape[0]
    vmem = pl.BlockSpec(memory_space=pltpu.VMEM)
    return pl.pallas_call(
        plan_kernel,
        out_shape=jax.ShapeDtypeStruct((8, n_dev), jnp.int32),
        in_specs=[vmem],
        out_specs=vmem,
        scratch_shapes=[pltpu.VMEM((n_dev, 32, n_dev), jnp.float32), pltpu.VMEM((n_dev, n_dev), jnp.float32)],
        name='plan_exchange')(block_table)


def store_kernel(ids_ref, kp_ref, vp_ref, kn_ref, vn_ref, ko_ref, vo_ref, kv_ref):
    def block(b, carry):
        ko_ref[b] = kp_ref[b]
        vo_ref[b] = vp_ref[b]
        kv_ref[b, 0] = jnp.swapaxes(kp_ref[b], 0, 1)
        kv_ref[b, 1] = jnp.swapaxes(vp_ref[b], 0, 1)
        return carry

    def write(i, carry):
        ko_ref[ids_ref[i]] = kn_ref[i]
        vo_ref[ids_ref[i]] = vn_ref[i]
        return carry

    lax.fori_loop(0, kp_ref.shape[0], block, 0)
    lax.fori_loop(0, kn_ref.shape[0], write, 0)


def store_chunk(k_pool, v_pool, k_new, v_new, write_ids):
    n_blocks, block_len, kv_heads, head_dim = k_pool.shape
    new_shape = (write_ids.size, block_len, kv_heads, head_dim)
    vmem = pl.BlockSpec(memory_space=pltpu.VMEM)
    return pl.pallas_call(
        store_kernel,
        out_shape=(jax.ShapeDtypeStruct(k_pool.shape, k_pool.dtype), jax.ShapeDtypeStruct(v_pool.shape, v_pool.dtype),
                   jax.ShapeDtypeStruct((n_blocks, 2, kv_heads, block_len, head_dim), k_pool.dtype)),
        in_specs=[pl.BlockSpec(memory_space=pltpu.SMEM)] + [vmem] * 4,
        out_specs=(vmem, vmem, vmem),
        name='store_chunk')(write_ids.reshape(-1), k_pool, v_pool, k_new.reshape(new_shape), v_new.reshape(new_shape))


def device_at(z, y, x, c):
    return z * 32 + y * 8 + x * 2 + c


def fused_kernel(plan_ref, q_ref, kn_ref, vn_ref, kv_ref, o_ref,
                 zbuf, cbuf, sbuf, wbuf, acc_ref, m_ref, l_ref, s0, s1, s2, s3, p0, p1, p2, p3, f0, f1, f2, f3,
                 z_send, z_recv, a_send, a_recv, b_send, b_recv, c_send, c_recv, w_send, w_recv):
    n_dev, kv_heads = 128, kn_ref.shape[0]
    heads = 4
    q_tile = q_ref.shape[1] // heads
    block_len = kv_ref.shape[3]
    scale = math.log2(math.e) * q_ref.shape[2] ** -0.5
    s_bufs, p_bufs, f_bufs = (s0, s1, s2, s3), (p0, p1, p2, p3), (f0, f1, f2, f3)
    me = lax.axis_index('pool')
    z, y, x, c = me // 32, (me // 8) % 4, (me // 2) % 4, me % 2
    col = me % 32
    other = device_at(z, y, x, 1 - c)
    sign = 1 + 2 * c

    def offset_peer(i):
        r = (i * 11) % 32
        dz = jnp.where(i < 32, 0, i % 3 + 1)
        return device_at((z + dz * sign) % 4, (y + (r // 8) * sign) % 4, (x + (r // 2) % 4 * sign) % 4, (c + r) % 2)

    barrier = pltpu.get_barrier_semaphore()

    def greet(i, carry):
        pl.semaphore_signal(barrier, inc=1, device_id=(offset_peer(i),), device_id_type=MESH)
        return carry

    lax.fori_loop(1, n_dev, greet, 0)

    for k in range(COMMON):
        zbuf[z * COMMON + k] = kv_ref[plan_ref[2, k]]

    def fill(i, carry):
        sbuf[i] = kv_ref[plan_ref[1, offset_peer(i)]]
        return carry

    def fill_group(group):
        lax.fori_loop(max(1, group * GROUP), (group + 1) * GROUP, fill, 0)

    fill_group(0)
    wbuf[0] = kv_ref[plan_ref[1, me]]
    pl.semaphore_wait(barrier, n_dev - 1)

    def remote(src, dst, ssem, rsem, peer):
        return pltpu.make_async_remote_copy(src_ref=src, dst_ref=dst, send_sem=ssem, recv_sem=rsem,
                                            device_id=(peer,), device_id_type=MESH)

    z_part = zbuf.at[pl.ds(z * COMMON, COMMON)]
    for s in range(1, 4):
        remote(z_part, z_part, z_send, z_recv, device_at((z + s) % 4, y, x, c)).start()

    def send_direct(group):
        def one(i, carry):
            remote(sbuf.at[i], wbuf.at[i], w_send.at[group], w_recv.at[group], offset_peer(i)).start()
            return carry
        lax.fori_loop(max(1, group * GROUP), (group + 1) * GROUP, one, 0)

    def direct_part(group):
        size = GROUP - 1 if group == 0 else GROUP
        part = wbuf.at[pl.ds(0, size)]
        return remote(part, part, w_send.at[group], w_recv.at[group], other)

    send_direct(0)

    row = lax.broadcasted_iota(jnp.int32, (kn_ref.shape[1], q_tile), 0)
    token = lax.broadcasted_iota(jnp.int32, (kn_ref.shape[1], q_tile), 1)

    def own_head(g, carry):
        for h in range(heads):
            cols = pl.ds(h * q_tile, q_tile)
            s = lax.dot_general(kn_ref[g], q_ref[g, cols, :], NT, preferred_element_type=jnp.float32)
            s = jnp.where(row <= token, s, -jnp.inf)
            top = jnp.max(s, axis=0, keepdims=True)
            e = jnp.exp2((s - top) * scale)
            m_ref[g, :, cols] = top
            l_ref[g, :, cols] = jnp.sum(e, axis=0, keepdims=True)
            acc_ref[g, :, cols] = lax.dot_general(vn_ref[g], e.astype(jnp.bfloat16), TN, preferred_element_type=jnp.float32)
        return carry

    lax.fori_loop(0, kv_heads, own_head, 0)
    for group in range(1, 4):
        fill_group(group)

    def attend(start):
        def rows_of(which, g):
            return wbuf[pl.ds(start, GROUP), which, g].reshape(GROUP * block_len, kv_ref.shape[4])

        def score(g, h):
            s_bufs[h][...] = lax.dot_general(rows_of(0, g), q_ref[g, pl.ds(h * q_tile, q_tile), :], NT, preferred_element_type=jnp.float32)

        def weigh(g, h):
            cols = pl.ds(h * q_tile, q_tile)
            old = m_ref[g, :, cols]
            top = jnp.maximum(old, jnp.max(s_bufs[h][...], axis=0, keepdims=True))
            fade = jnp.exp2((old - top) * scale)
            e = jnp.exp2((s_bufs[h][...] - top) * scale)
            l_ref[g, :, cols] = l_ref[g, :, cols] * fade + jnp.sum(e, axis=0, keepdims=True)
            p_bufs[h][...] = e.astype(jnp.bfloat16)
            m_ref[g, :, cols] = top
            f_bufs[h][...] = fade

        def add_values(g, h):
            cols = pl.ds(h * q_tile, q_tile)
            part = lax.dot_general(rows_of(1, g), p_bufs[h][...], TN, preferred_element_type=jnp.float32)
            acc_ref[g, :, cols] = acc_ref[g, :, cols] * f_bufs[h][...] + part

        for h in range(heads):
            score(0, h)
        p_bufs[heads - 1][...] = jnp.zeros_like(p_bufs[heads - 1])
        f_bufs[heads - 1][...] = jnp.ones_like(f_bufs[heads - 1])

        def per_group(g, carry):
            following, last = jnp.minimum(g + 1, kv_heads - 1), jnp.maximum(g - 1, 0)
            for h in range(heads):
                if h == 0:
                    add_values(last, heads - 1)
                else:
                    add_values(g, h - 1)
                weigh(g, h)
                score(following, h)
            return carry

        lax.fori_loop(0, kv_heads, per_group, 0)
        add_values(kv_heads - 1, heads - 1)

    y_first = 1 - c

    def peer_a(s):
        return device_at(z, (y + s * y_first) % 4, (x + s * (1 - y_first)) % 4, c)

    def peer_b(s):
        return device_at(z, (y + s * (1 - y_first)) % 4, (x + s * y_first) % 4, c)

    def line_column(yy, xx):
        return (yy % 4) * 8 + (xx % 4) * 2 + c

    def part_of(column):
        return cbuf.at[pl.ds(column * COMMON, COMMON)]

    own_part = part_of(col)
    three = cbuf.at[pl.ds(0, 3 * COMMON)]
    four = cbuf.at[pl.ds(0, 4 * COMMON)]
    z_three = zbuf.at[pl.ds(0, 3 * COMMON)]
    lines = [part_of(line_column(y + i * y_first, x + i * (1 - y_first))) for i in range(4)]

    remote(z_three, z_three, z_send, z_recv, other).wait_recv()
    for k in range(COMMON):
        cbuf[col * COMMON + k] = zbuf[plan_ref[3, k]]
    for s in range(1, 4):
        remote(own_part, own_part, a_send, a_recv, peer_a(s)).start()
    remote(own_part, own_part, c_send.at[0], c_recv.at[0], other).start()
    send_direct(1)
    remote(three, three, a_send, a_recv, other).wait_recv()
    for s in range(1, 4):
        for line in lines:
            remote(line, line, b_send, b_recv.at[s - 1], peer_b(s)).start()
    for line in lines[1:]:
        remote(line, line, c_send.at[0], c_recv.at[0], other).start()
    send_direct(2)
    send_direct(3)

    def step(t, carry):
        for group in range(3):
            @pl.when(t == group)
            def _(group=group):
                direct_part(group).wait_recv()

        @pl.when(t == 2)
        def _():
            for s in range(1, 4):
                remote(four, four, b_send, b_recv.at[s - 1], other).wait_recv()
                for i in range(4):
                    line = part_of(line_column(y + i * y_first - s * (1 - y_first), x + i * (1 - y_first) - s * y_first))
                    remote(line, line, c_send.at[s], c_recv.at[s], other).start()

        @pl.when(t == 3)
        def _():
            for s in range(4):
                remote(four, four, c_send.at[s], c_recv.at[s], other).wait_recv()

        @pl.when((t >= 3) & (t < 7))
        def _():
            def pick(i, inner):
                wbuf[n_dev + i] = cbuf[plan_ref[4, (t - 3) * GROUP + i]]
                return inner
            lax.fori_loop(0, GROUP, pick, 0)

        @pl.when(t == 7)
        def _():
            direct_part(3).wait_recv()

        attend(jnp.where(t < 3, t, jnp.where(t < 7, 4, 3)) * GROUP)
        return carry

    lax.fori_loop(0, 8, step, 0)

    def finish(g, carry):
        for h in range(heads):
            cols = pl.ds(h * q_tile, q_tile)
            out = acc_ref[g, :, cols] / l_ref[g, :, cols]
            o_ref[g, cols, :] = out.T.astype(jnp.bfloat16)
        return carry

    lax.fori_loop(0, kv_heads, finish, 0)
    remote(z_three, z_three, z_send, z_recv, other).wait_send()
    remote(three, three, a_send, a_recv, other).wait_send()
    twelve = cbuf.at[pl.ds(0, 12 * COMMON)]
    remote(twelve, twelve, b_send, b_recv.at[0], other).wait_send()
    for s in range(4):
        remote(four, four, c_send.at[s], c_recv.at[s], other).wait_send()
    for group in range(4):
        direct_part(group).wait_send()


def fused_attention(queries, k_new, v_new, kv, plan):
    _, chunk_len, q_heads, head_dim = queries.shape
    kv_heads = k_new.shape[2]
    q_grp = queries[0].transpose(1, 0, 2).reshape(kv_heads, -1, head_dim)
    k_own, v_own = k_new[0].transpose(1, 0, 2), v_new[0].transpose(1, 0, 2)
    block = kv.shape[1:]
    q_rows, q_tile = q_grp.shape[1], q_grp.shape[1] // 4
    keys = GROUP * block[2]
    bf16, f32 = jnp.bfloat16, jnp.float32
    smem, vmem = pl.BlockSpec(memory_space=pltpu.SMEM), pl.BlockSpec(memory_space=pltpu.VMEM)
    dma = pltpu.SemaphoreType.DMA
    out = pl.pallas_call(
        fused_kernel,
        out_shape=jax.ShapeDtypeStruct(q_grp.shape, bf16),
        in_specs=[smem] + [vmem] * 4,
        out_specs=vmem,
        scratch_shapes=[
            pltpu.VMEM((4 * COMMON,) + block, bf16),
            pltpu.VMEM((32 * COMMON,) + block, bf16),
            pltpu.VMEM((128,) + block, bf16),
            pltpu.VMEM((128 + GROUP,) + block, bf16),
            pltpu.VMEM((kv_heads, head_dim, q_rows), f32),
            pltpu.VMEM((kv_heads, 1, q_rows), f32),
            pltpu.VMEM((kv_heads, 1, q_rows), f32)]
        + [pltpu.VMEM((keys, q_tile), f32)] * 4 + [pltpu.VMEM((keys, q_tile), bf16)] * 4 + [pltpu.VMEM((1, q_tile), f32)] * 4
        + [dma, dma, dma, dma, dma, dma((3,)), dma((4,)), dma((4,)), dma((4,)), dma((4,))],
        compiler_params=pltpu.CompilerParams(has_side_effects=True, collective_id=0, vmem_limit_bytes=66_000_000),
        name='fused_attention')(plan, q_grp, k_own, v_own, kv)
    return out.reshape(q_heads, chunk_len, head_dim)


def solution(mesh):
    n_dev = mesh.shape['pool']

    def local_step(queries, k_new, v_new, k_pool, v_pool, block_table, write_ids):
        plan = plan_exchange(block_table)
        k_pool_out, v_pool_out, kv = store_chunk(k_pool, v_pool, k_new, v_new, write_ids)
        by_head = lax.cond(
            plan[0, 0] == 0,
            lambda: fused_attention(queries, k_new, v_new, kv, plan),
            lambda: general_attention(n_dev, queries, k_new, v_new, k_pool, v_pool, block_table)[0].transpose(1, 0, 2))
        return by_head.transpose(1, 0, 2)[None], k_pool_out, v_pool_out

    row_spec = P('pool')
    return jax.shard_map(local_step, mesh=mesh, in_specs=(row_spec, row_spec, row_spec, row_spec, row_spec, P(), row_spec), out_specs=(row_spec, row_spec, row_spec), check_vma=False)
```

```python
import functools
import math

import jax
import jax.numpy as jnp
from jax import lax
from jax.experimental import pallas as pl
from jax.experimental.pallas import tpu as pltpu
from jax.sharding import PartitionSpec as P

COMMON = 8
GROUP = 32
MESH = pl.DeviceIdType.MESH


def chunk_attention(q_grp, k_pref, v_pref, k_chunk, v_chunk):
    chunk_len = q_grp.shape[1]
    score_scale = q_grp.shape[-1] ** -0.5
    s_pref = jnp.einsum('rcgqd,rtgd->rcgqt', q_grp, k_pref, preferred_element_type=jnp.float32) * score_scale
    s_self = jnp.einsum('rcgqd,rtgd->rcgqt', q_grp, k_chunk, preferred_element_type=jnp.float32) * score_scale
    causal = (jnp.arange(chunk_len)[:, None] >= jnp.arange(chunk_len)[None, :])[None, :, None, None, :]
    s_self = jnp.where(causal, s_self, -jnp.inf)
    row_max = jnp.maximum(jnp.max(s_pref, axis=-1), jnp.max(s_self, axis=-1))[..., None]
    e_pref = jnp.exp(s_pref - row_max)
    e_self = jnp.exp(s_self - row_max)
    prob_total = jnp.sum(e_pref, axis=-1, keepdims=True) + jnp.sum(e_self, axis=-1, keepdims=True)
    p_pref = (e_pref / prob_total).astype(jnp.bfloat16)
    p_self = (e_self / prob_total).astype(jnp.bfloat16)
    attn_acc = jnp.einsum('rcgqt,rtgd->rcgqd', p_pref, v_pref, preferred_element_type=jnp.float32)
    return attn_acc + jnp.einsum('rcgqt,rtgd->rcgqd', p_self, v_chunk, preferred_element_type=jnp.float32)


def general_attention(n_dev, queries, k_new, v_new, k_pool, v_pool, block_table):
    req_count, chunk_len, q_heads, head_dim = queries.shape
    kv_heads = k_new.shape[2]
    per_dev, block_len = k_pool.shape[0], k_pool.shape[1]
    n_pref = block_table.shape[1]
    row_cap = 2 * n_pref // n_dev + (n_pref // 2 + n_dev - 1) // n_dev
    pair_cap = req_count * row_cap
    my_index = lax.axis_index('pool')
    owners = block_table // per_dev
    owned_here = (owners == my_index).reshape(n_dev, req_count * n_pref).astype(jnp.int32)
    send_slot = jnp.where(owned_here > 0, jnp.cumsum(owned_here, axis=1) - 1, pair_cap)
    dest_dev = jnp.broadcast_to(jnp.arange(n_dev)[:, None], send_slot.shape)
    local_ids = (block_table % per_dev).reshape(n_dev, req_count * n_pref)
    send_ids = jnp.zeros((n_dev, pair_cap), jnp.int32).at[dest_dev, send_slot].set(local_ids, mode='drop')
    k_recv = lax.all_to_all(k_pool[send_ids], 'pool', 0, 0, tiled=True)
    v_recv = lax.all_to_all(v_pool[send_ids], 'pool', 0, 0, tiled=True)
    my_owners = lax.dynamic_slice_in_dim(owners, my_index * req_count, req_count, 0).reshape(-1)
    from_owner = (my_owners[:, None] == jnp.arange(n_dev)[None, :]).astype(jnp.int32)
    slot_rank = jnp.sum(from_owner * (jnp.cumsum(from_owner, axis=0) - 1), axis=1)
    recv_idx = (my_owners * pair_cap + slot_rank).reshape(req_count, n_pref)
    flat_shape = (n_dev * pair_cap, block_len, kv_heads, head_dim)
    prefix_shape = (req_count, n_pref * block_len, kv_heads, head_dim)
    k_pref = k_recv.reshape(flat_shape)[recv_idx].reshape(prefix_shape)
    v_pref = v_recv.reshape(flat_shape)[recv_idx].reshape(prefix_shape)
    q_grp = queries.reshape(req_count, chunk_len, kv_heads, q_heads // kv_heads, head_dim)
    attn_acc = chunk_attention(q_grp, k_pref, v_pref, k_new, v_new)
    return attn_acc.reshape(req_count, chunk_len, q_heads, head_dim).astype(jnp.bfloat16)


NT = (((1,), (1,)), ((), ()))
TN = (((0,), (0,)), ((), ()))


def plan_kernel(tab_ref, plan_ref, named_ref, least_ref):
    f32, bf16, i32 = jnp.float32, jnp.bfloat16, jnp.int32
    n_dev, n_pref = tab_ref.shape
    per_dev, n_col = 32, n_dev // 4
    me = lax.axis_index('pool')
    none = 1e6

    def iota(shape, dim):
        return lax.broadcasted_iota(i32, shape, dim)

    def ones(mask):
        return jnp.where(mask, 1.0, 0.0).astype(f32)

    def dot(a, b, dims=(((1,), (0,)), ((), ()))):
        return lax.dot_general(a.astype(bf16), b.astype(bf16), dims, preferred_element_type=f32)

    local_row = iota((per_dev, n_pref), 0)
    owner_row = iota((n_dev, n_pref), 0)
    local = iota((per_dev, n_dev), 0)
    owner = iota((per_dev, n_dev), 1)

    def count_row(r, total):
        row = tab_ref[pl.ds(r, 1), :]
        named = dot(ones(local_row == row % per_dev), ones(owner_row == row // per_dev), NT)
        named_ref[r] = named
        return total + named

    use_count = lax.fori_loop(0, n_dev, count_row, jnp.zeros((per_dev, n_dev), f32), unroll=8)
    order = use_count * per_dev + local.astype(f32)

    def split_row(r, carry):
        common, worst = carry
        named = named_ref[r] > 0
        key = jnp.where(named, order, none)
        least = jnp.min(key, axis=0, keepdims=True)
        least_ref[pl.ds(r, 1), :] = least
        common = jnp.maximum(common, ones(named & (key > least)))
        return common, jnp.maximum(worst, least)

    common, worst = lax.fori_loop(0, n_dev, split_row, (jnp.zeros((per_dev, n_dev), f32), jnp.zeros((1, n_dev), f32)), unroll=8)
    tri = ones(iota((per_dev, per_dev), 0) > iota((per_dev, per_dev), 1))
    rank = dot(tri, common)
    one_row = jnp.ones((8, per_dev), f32)
    source, target = iota((n_dev, n_dev), 0), iota((n_dev, n_dev), 1)
    per_owner = dot(one_row, common)
    same_col = source % n_col == target % n_col
    base = dot(per_owner, ones(same_col & (source < target)))[:1]
    in_all = dot(per_owner, ones(same_col))[:1]
    misfit = jnp.maximum(jnp.max(ones(worst >= none)), jnp.max(ones(in_all > COMMON)))
    in_col = base + rank
    slot = (owner % n_col * COMMON).astype(f32) + in_col
    pick_me = ones(iota((8, n_dev), 1) == me)
    direct = dot(pick_me, (least_ref[...].astype(i32) % per_dev).astype(f32), NT)[:1]
    here = owner == me
    my_common = jnp.sum(jnp.where(here, common, 0.0), axis=1, keepdims=True)
    my_rank = jnp.sum(jnp.where(here, rank, 0.0), axis=1, keepdims=True)
    lane = owner.astype(f32)
    own = jnp.sum(jnp.where((my_common > 0) & (my_rank == lane), local.astype(f32), 0.0), axis=0, keepdims=True)
    in_my_col = (common > 0) & (owner % n_col == me % n_col)
    place_in_z = (owner // n_col * COMMON).astype(f32) + rank
    lane_row = iota((1, n_dev), 1)
    col = jnp.zeros((1, n_dev), f32)
    for k in range(COMMON):
        found = jnp.sum(jnp.where(in_my_col & (in_col == k), place_in_z, 0.0))
        col = jnp.where(lane_row == k, found, col)
    mine = named_ref[me] * common
    before = dot(dot(one_row, mine), ones(source < target))[:1]
    place = jnp.where(mine > 0, dot(tri, mine) + before, -1.0).T
    slot_t = slot.T
    j_lane = target.astype(f32)
    pick = jnp.zeros((n_dev, n_dev), f32)
    for l in range(per_dev):
        pick = pick + jnp.where(place[:, l:l + 1] == j_lane, slot_t[:, l:l + 1], 0.0)
    pick = jnp.sum(pick, axis=0, keepdims=True)
    plan_ref[...] = jnp.zeros(plan_ref.shape, i32)
    for i, value in enumerate((misfit + jnp.zeros((1, n_dev), f32), direct, own, col, pick)):
        plan_ref[i:i + 1, :] = value.astype(i32)


def plan_exchange(block_table):
    n_dev = block_table.shape[0]
    vmem = pl.BlockSpec(memory_space=pltpu.VMEM)
    return pl.pallas_call(
        plan_kernel,
        out_shape=jax.ShapeDtypeStruct((8, n_dev), jnp.int32),
        in_specs=[vmem],
        out_specs=vmem,
        scratch_shapes=[pltpu.VMEM((n_dev, 32, n_dev), jnp.float32), pltpu.VMEM((n_dev, n_dev), jnp.float32)],
        name='plan_exchange')(block_table)


def store_kernel(ids_ref, kp_ref, vp_ref, kn_ref, vn_ref, ko_ref, vo_ref, kv_ref):
    def block(b, carry):
        ko_ref[b] = kp_ref[b]
        vo_ref[b] = vp_ref[b]
        kv_ref[b, 0] = jnp.swapaxes(kp_ref[b], 0, 1)
        kv_ref[b, 1] = jnp.swapaxes(vp_ref[b], 0, 1)
        return carry

    def write(i, carry):
        ko_ref[ids_ref[i]] = kn_ref[i]
        vo_ref[ids_ref[i]] = vn_ref[i]
        return carry

    lax.fori_loop(0, kp_ref.shape[0], block, 0)
    lax.fori_loop(0, kn_ref.shape[0], write, 0)


def store_chunk(k_pool, v_pool, k_new, v_new, write_ids):
    n_blocks, block_len, kv_heads, head_dim = k_pool.shape
    new_shape = (write_ids.size, block_len, kv_heads, head_dim)
    vmem = pl.BlockSpec(memory_space=pltpu.VMEM)
    return pl.pallas_call(
        store_kernel,
        out_shape=(jax.ShapeDtypeStruct(k_pool.shape, k_pool.dtype), jax.ShapeDtypeStruct(v_pool.shape, v_pool.dtype),
                   jax.ShapeDtypeStruct((n_blocks, 2, kv_heads, block_len, head_dim), k_pool.dtype)),
        in_specs=[pl.BlockSpec(memory_space=pltpu.SMEM)] + [vmem] * 4,
        out_specs=(vmem, vmem, vmem),
        name='store_chunk')(write_ids.reshape(-1), k_pool, v_pool, k_new.reshape(new_shape), v_new.reshape(new_shape))


def device_at(z, y, x, c):
    return z * 32 + y * 8 + x * 2 + c


def fused_kernel(plan_ref, q_ref, kn_ref, vn_ref, kv_ref, o_ref,
                 zbuf, cbuf, sbuf, wbuf, acc_ref, m_ref, l_ref, s0, s1, s2, s3, p0, p1, p2, p3, f0, f1, f2, f3,
                 z_send, z_recv, a_send, a_recv, b_send, b_recv, c_send, c_recv, w_send, w_recv):
    n_dev, kv_heads = 128, kn_ref.shape[0]
    heads = 4
    q_tile = q_ref.shape[1] // heads
    block_len = kv_ref.shape[3]
    scale = math.log2(math.e) * q_ref.shape[2] ** -0.5
    s_bufs, p_bufs, f_bufs = (s0, s1, s2, s3), (p0, p1, p2, p3), (f0, f1, f2, f3)
    me = lax.axis_index('pool')
    z, y, x, c = me // 32, (me // 8) % 4, (me // 2) % 4, me % 2
    col = me % 32
    other = device_at(z, y, x, 1 - c)
    sign = 1 + 2 * c

    def offset_peer(i):
        r = (i * 11) % 32
        dz = jnp.where(i < 32, 0, i % 3 + 1)
        return device_at((z + dz * sign) % 4, (y + (r // 8) * sign) % 4, (x + (r // 2) % 4 * sign) % 4, (c + r) % 2)

    barrier = pltpu.get_barrier_semaphore()

    def greet(i, carry):
        pl.semaphore_signal(barrier, inc=1, device_id=(offset_peer(i),), device_id_type=MESH)
        return carry

    lax.fori_loop(1, n_dev, greet, 0)

    for k in range(COMMON):
        zbuf[z * COMMON + k] = kv_ref[plan_ref[2, k]]

    def fill(i, carry):
        sbuf[i] = kv_ref[plan_ref[1, offset_peer(i)]]
        return carry

    def fill_group(group):
        lax.fori_loop(max(1, group * GROUP), (group + 1) * GROUP, fill, 0)

    fill_group(0)
    wbuf[0] = kv_ref[plan_ref[1, me]]
    pl.semaphore_wait(barrier, n_dev - 1)

    def remote(src, dst, ssem, rsem, peer):
        return pltpu.make_async_remote_copy(src_ref=src, dst_ref=dst, send_sem=ssem, recv_sem=rsem,
                                            device_id=(peer,), device_id_type=MESH)

    z_part = zbuf.at[pl.ds(z * COMMON, COMMON)]
    for s in range(1, 4):
        remote(z_part, z_part, z_send, z_recv, device_at((z + s) % 4, y, x, c)).start()

    def send_direct(group):
        def one(i, carry):
            remote(sbuf.at[i], wbuf.at[i], w_send.at[group], w_recv.at[group], offset_peer(i)).start()
            return carry
        lax.fori_loop(max(1, group * GROUP), (group + 1) * GROUP, one, 0)

    def direct_part(group):
        size = GROUP - 1 if group == 0 else GROUP
        part = wbuf.at[pl.ds(0, size)]
        return remote(part, part, w_send.at[group], w_recv.at[group], other)

    send_direct(0)

    row = lax.broadcasted_iota(jnp.int32, (kn_ref.shape[1], q_tile), 0)
    token = lax.broadcasted_iota(jnp.int32, (kn_ref.shape[1], q_tile), 1)

    def own_head(g, carry):
        for h in range(heads):
            cols = pl.ds(h * q_tile, q_tile)
            s = lax.dot_general(kn_ref[g], q_ref[g, cols, :], NT, preferred_element_type=jnp.float32)
            s = jnp.where(row <= token, s, -jnp.inf)
            top = jnp.max(s, axis=0, keepdims=True)
            e = jnp.exp2((s - top) * scale)
            m_ref[g, :, cols] = top
            l_ref[g, :, cols] = jnp.sum(e, axis=0, keepdims=True)
            acc_ref[g, :, cols] = lax.dot_general(vn_ref[g], e.astype(jnp.bfloat16), TN, preferred_element_type=jnp.float32)
        return carry

    lax.fori_loop(0, kv_heads, own_head, 0)
    for group in range(1, 4):
        fill_group(group)

    def attend(start):
        def rows_of(which, g):
            return wbuf[pl.ds(start, GROUP), which, g].reshape(GROUP * block_len, kv_ref.shape[4])

        def score(g, h):
            s_bufs[h][...] = lax.dot_general(rows_of(0, g), q_ref[g, pl.ds(h * q_tile, q_tile), :], NT, preferred_element_type=jnp.float32)

        def weigh(g, h):
            cols = pl.ds(h * q_tile, q_tile)
            old = m_ref[g, :, cols]
            top = jnp.maximum(old, jnp.max(s_bufs[h][...], axis=0, keepdims=True))
            fade = jnp.exp2((old - top) * scale)
            e = jnp.exp2((s_bufs[h][...] - top) * scale)
            l_ref[g, :, cols] = l_ref[g, :, cols] * fade + jnp.sum(e, axis=0, keepdims=True)
            p_bufs[h][...] = e.astype(jnp.bfloat16)
            m_ref[g, :, cols] = top
            f_bufs[h][...] = fade

        def add_values(g, h):
            cols = pl.ds(h * q_tile, q_tile)
            part = lax.dot_general(rows_of(1, g), p_bufs[h][...], TN, preferred_element_type=jnp.float32)
            acc_ref[g, :, cols] = acc_ref[g, :, cols] * f_bufs[h][...] + part

        for h in range(heads):
            score(0, h)
        p_bufs[heads - 1][...] = jnp.zeros_like(p_bufs[heads - 1])
        f_bufs[heads - 1][...] = jnp.ones_like(f_bufs[heads - 1])

        def per_group(g, carry):
            following, last = jnp.minimum(g + 1, kv_heads - 1), jnp.maximum(g - 1, 0)
            for h in range(heads):
                if h == 0:
                    add_values(last, heads - 1)
                else:
                    add_values(g, h - 1)
                weigh(g, h)
                score(following, h)
            return carry

        lax.fori_loop(0, kv_heads, per_group, 0)
        add_values(kv_heads - 1, heads - 1)

    y_first = 1 - c

    def line_at(first, second):
        yy = (y + first * y_first + second * (1 - y_first)) % 4
        xx = (x + first * (1 - y_first) + second * y_first) % 4
        return (yy * 8 + xx * 2 + c) * COMMON

    def peer_at(first, second):
        yy = (y + first * y_first + second * (1 - y_first)) % 4
        xx = (x + first * (1 - y_first) + second * y_first) % 4
        return device_at(z, yy, xx, c)

    next_a, prev_a, next_b, prev_b = peer_at(1, 0), peer_at(3, 0), peer_at(0, 1), peer_at(0, 3)
    half = COMMON // 2

    def share(start, size, ssem, rsem, peer):
        part = cbuf.at[pl.ds(start, size)]
        return remote(part, part, ssem, rsem, peer)

    def arrived(blocks, ssem, rsem):
        share(0, blocks, ssem, rsem, other).wait_recv()

    def to_second(i, first):
        start = line_at(first, 0)
        share(start, COMMON, b_send, b_recv.at[3 * i], next_b).start()
        share(start, COMMON, b_send, b_recv.at[3 * i + 1], prev_b).start()
        share(start, COMMON, c_send.at[0], c_recv.at[0], other).start()

    z_three = zbuf.at[pl.ds(0, 3 * COMMON)]
    order = (0, 3, 1, 2)

    remote(z_three, z_three, z_send, z_recv, other).wait_recv()
    for k in range(COMMON):
        cbuf[col * COMMON + k] = zbuf[plan_ref[3, k]]
    share(line_at(0, 0), COMMON, a_send, a_recv.at[0], next_a).start()
    share(line_at(0, 0), COMMON, a_send, a_recv.at[1], prev_a).start()
    to_second(0, 0)
    arrived(COMMON, a_send, a_recv.at[0])
    share(line_at(3, 0), half, a_send, a_recv.at[2], next_a).start()
    to_second(1, 3)
    arrived(COMMON, a_send, a_recv.at[1])
    share(line_at(1, 0) + half, half, a_send, a_recv.at[2], prev_a).start()
    to_second(2, 1)
    arrived(COMMON, a_send, a_recv.at[2])
    to_second(3, 2)
    for i, first in enumerate(order):
        arrived(COMMON, b_send, b_recv.at[3 * i])
        share(line_at(first, 3), half, b_send, b_recv.at[3 * i + 2], next_b).start()
        share(line_at(first, 3), COMMON, c_send.at[1], c_recv.at[1], other).start()
        arrived(COMMON, b_send, b_recv.at[3 * i + 1])
        share(line_at(first, 1) + half, half, b_send, b_recv.at[3 * i + 2], prev_b).start()
        share(line_at(first, 1), COMMON, c_send.at[2], c_recv.at[2], other).start()
    for group in range(1, 4):
        send_direct(group)
    for i, first in enumerate(order):
        arrived(COMMON, b_send, b_recv.at[3 * i + 2])
        share(line_at(first, 2), COMMON, c_send.at[3], c_recv.at[3], other).start()

    def step(t, carry):
        @pl.when(t == 0)
        def _():
            direct_part(0).wait_recv()

        @pl.when(t == 1)
        def _():
            for i in range(4):
                arrived(4 * COMMON, c_send.at[i], c_recv.at[i])

        @pl.when((t >= 1) & (t < 5))
        def _():
            def pick(i, inner):
                wbuf[n_dev + i] = cbuf[plan_ref[4, (t - 1) * GROUP + i]]
                return inner
            lax.fori_loop(0, GROUP, pick, 0)

        for group in range(1, 4):
            @pl.when(t == group + 4)
            def _(group=group):
                direct_part(group).wait_recv()

        attend(jnp.where(t < 1, 0, jnp.where(t < 5, 4, t - 4)) * GROUP)
        return carry

    lax.fori_loop(0, 8, step, 0)

    def finish(g, carry):
        for h in range(heads):
            cols = pl.ds(h * q_tile, q_tile)
            out = acc_ref[g, :, cols] / l_ref[g, :, cols]
            o_ref[g, cols, :] = out.T.astype(jnp.bfloat16)
        return carry

    lax.fori_loop(0, kv_heads, finish, 0)
    remote(z_three, z_three, z_send, z_recv, other).wait_send()
    share(0, 3 * COMMON, a_send, a_recv.at[0], other).wait_send()
    share(0, 12 * COMMON, b_send, b_recv.at[0], other).wait_send()
    for i in range(4):
        share(0, 4 * COMMON, c_send.at[i], c_recv.at[i], other).wait_send()
    for group in range(4):
        direct_part(group).wait_send()


def fused_attention(queries, k_new, v_new, kv, plan):
    _, chunk_len, q_heads, head_dim = queries.shape
    kv_heads = k_new.shape[2]
    q_grp = queries[0].transpose(1, 0, 2).reshape(kv_heads, -1, head_dim)
    k_own, v_own = k_new[0].transpose(1, 0, 2), v_new[0].transpose(1, 0, 2)
    block = kv.shape[1:]
    q_rows, q_tile = q_grp.shape[1], q_grp.shape[1] // 4
    keys = GROUP * block[2]
    bf16, f32 = jnp.bfloat16, jnp.float32
    smem, vmem = pl.BlockSpec(memory_space=pltpu.SMEM), pl.BlockSpec(memory_space=pltpu.VMEM)
    dma = pltpu.SemaphoreType.DMA
    out = pl.pallas_call(
        fused_kernel,
        out_shape=jax.ShapeDtypeStruct(q_grp.shape, bf16),
        in_specs=[smem] + [vmem] * 4,
        out_specs=vmem,
        scratch_shapes=[
            pltpu.VMEM((4 * COMMON,) + block, bf16),
            pltpu.VMEM((32 * COMMON,) + block, bf16),
            pltpu.VMEM((128,) + block, bf16),
            pltpu.VMEM((128 + GROUP,) + block, bf16),
            pltpu.VMEM((kv_heads, head_dim, q_rows), f32),
            pltpu.VMEM((kv_heads, 1, q_rows), f32),
            pltpu.VMEM((kv_heads, 1, q_rows), f32)]
        + [pltpu.VMEM((keys, q_tile), f32)] * 4 + [pltpu.VMEM((keys, q_tile), bf16)] * 4 + [pltpu.VMEM((1, q_tile), f32)] * 4
        + [dma, dma, dma, dma((3,)), dma, dma((12,)), dma((4,)), dma((4,)), dma((4,)), dma((4,))],
        compiler_params=pltpu.CompilerParams(has_side_effects=True, collective_id=0, vmem_limit_bytes=66_000_000),
        name='fused_attention')(plan, q_grp, k_own, v_own, kv)
    return out.reshape(q_heads, chunk_len, head_dim)


def solution(mesh):
    n_dev = mesh.shape['pool']

    def local_step(queries, k_new, v_new, k_pool, v_pool, block_table, write_ids):
        plan = plan_exchange(block_table)
        k_pool_out, v_pool_out, kv = store_chunk(k_pool, v_pool, k_new, v_new, write_ids)
        by_head = lax.cond(
            plan[0, 0] == 0,
            lambda: fused_attention(queries, k_new, v_new, kv, plan),
            lambda: general_attention(n_dev, queries, k_new, v_new, k_pool, v_pool, block_table)[0].transpose(1, 0, 2))
        return by_head.transpose(1, 0, 2)[None], k_pool_out, v_pool_out

    row_spec = P('pool')
    return jax.shard_map(local_step, mesh=mesh, in_specs=(row_spec, row_spec, row_spec, row_spec, row_spec, P(), row_spec), out_specs=(row_spec, row_spec, row_spec), check_vma=False)
```

```python
import functools
import math

import jax
import jax.numpy as jnp
from jax import lax
from jax.experimental import pallas as pl
from jax.experimental.pallas import tpu as pltpu
from jax.sharding import PartitionSpec as P

COMMON = 8
GROUP = 32
MESH = pl.DeviceIdType.MESH
PLACES = (0, 1, 3, 4, 12, 5, 15, 2, 8, 7, 13, 6, 9, 14, 11, 10)


def chunk_attention(q_grp, k_pref, v_pref, k_chunk, v_chunk):
    chunk_len = q_grp.shape[1]
    score_scale = q_grp.shape[-1] ** -0.5
    s_pref = jnp.einsum('rcgqd,rtgd->rcgqt', q_grp, k_pref, preferred_element_type=jnp.float32) * score_scale
    s_self = jnp.einsum('rcgqd,rtgd->rcgqt', q_grp, k_chunk, preferred_element_type=jnp.float32) * score_scale
    causal = (jnp.arange(chunk_len)[:, None] >= jnp.arange(chunk_len)[None, :])[None, :, None, None, :]
    s_self = jnp.where(causal, s_self, -jnp.inf)
    row_max = jnp.maximum(jnp.max(s_pref, axis=-1), jnp.max(s_self, axis=-1))[..., None]
    e_pref = jnp.exp(s_pref - row_max)
    e_self = jnp.exp(s_self - row_max)
    prob_total = jnp.sum(e_pref, axis=-1, keepdims=True) + jnp.sum(e_self, axis=-1, keepdims=True)
    p_pref = (e_pref / prob_total).astype(jnp.bfloat16)
    p_self = (e_self / prob_total).astype(jnp.bfloat16)
    attn_acc = jnp.einsum('rcgqt,rtgd->rcgqd', p_pref, v_pref, preferred_element_type=jnp.float32)
    return attn_acc + jnp.einsum('rcgqt,rtgd->rcgqd', p_self, v_chunk, preferred_element_type=jnp.float32)


def general_attention(n_dev, queries, k_new, v_new, k_pool, v_pool, block_table):
    req_count, chunk_len, q_heads, head_dim = queries.shape
    kv_heads = k_new.shape[2]
    per_dev, block_len = k_pool.shape[0], k_pool.shape[1]
    n_pref = block_table.shape[1]
    row_cap = 2 * n_pref // n_dev + (n_pref // 2 + n_dev - 1) // n_dev
    pair_cap = req_count * row_cap
    my_index = lax.axis_index('pool')
    owners = block_table // per_dev
    owned_here = (owners == my_index).reshape(n_dev, req_count * n_pref).astype(jnp.int32)
    send_slot = jnp.where(owned_here > 0, jnp.cumsum(owned_here, axis=1) - 1, pair_cap)
    dest_dev = jnp.broadcast_to(jnp.arange(n_dev)[:, None], send_slot.shape)
    local_ids = (block_table % per_dev).reshape(n_dev, req_count * n_pref)
    send_ids = jnp.zeros((n_dev, pair_cap), jnp.int32).at[dest_dev, send_slot].set(local_ids, mode='drop')
    k_recv = lax.all_to_all(k_pool[send_ids], 'pool', 0, 0, tiled=True)
    v_recv = lax.all_to_all(v_pool[send_ids], 'pool', 0, 0, tiled=True)
    my_owners = lax.dynamic_slice_in_dim(owners, my_index * req_count, req_count, 0).reshape(-1)
    from_owner = (my_owners[:, None] == jnp.arange(n_dev)[None, :]).astype(jnp.int32)
    slot_rank = jnp.sum(from_owner * (jnp.cumsum(from_owner, axis=0) - 1), axis=1)
    recv_idx = (my_owners * pair_cap + slot_rank).reshape(req_count, n_pref)
    flat_shape = (n_dev * pair_cap, block_len, kv_heads, head_dim)
    prefix_shape = (req_count, n_pref * block_len, kv_heads, head_dim)
    k_pref = k_recv.reshape(flat_shape)[recv_idx].reshape(prefix_shape)
    v_pref = v_recv.reshape(flat_shape)[recv_idx].reshape(prefix_shape)
    q_grp = queries.reshape(req_count, chunk_len, kv_heads, q_heads // kv_heads, head_dim)
    attn_acc = chunk_attention(q_grp, k_pref, v_pref, k_new, v_new)
    return attn_acc.reshape(req_count, chunk_len, q_heads, head_dim).astype(jnp.bfloat16)


NT = (((1,), (1,)), ((), ()))
TN = (((0,), (0,)), ((), ()))


def plan_kernel(tab_ref, plan_ref, named_ref, least_ref):
    f32, bf16, i32 = jnp.float32, jnp.bfloat16, jnp.int32
    n_dev, n_pref = tab_ref.shape
    per_dev, n_col = 32, n_dev // 4
    me = lax.axis_index('pool')
    none = 1e6

    def iota(shape, dim):
        return lax.broadcasted_iota(i32, shape, dim)

    def ones(mask):
        return jnp.where(mask, 1.0, 0.0).astype(f32)

    def dot(a, b, dims=(((1,), (0,)), ((), ()))):
        return lax.dot_general(a.astype(bf16), b.astype(bf16), dims, preferred_element_type=f32)

    local_row = iota((per_dev, n_pref), 0)
    owner_row = iota((n_dev, n_pref), 0)
    local = iota((per_dev, n_dev), 0)
    owner = iota((per_dev, n_dev), 1)

    def count_row(r, total):
        row = tab_ref[pl.ds(r, 1), :]
        named = dot(ones(local_row == row % per_dev), ones(owner_row == row // per_dev), NT)
        named_ref[r] = named
        return total + named

    use_count = lax.fori_loop(0, n_dev, count_row, jnp.zeros((per_dev, n_dev), f32), unroll=8)
    order = use_count * per_dev + local.astype(f32)

    def split_row(r, carry):
        common, worst = carry
        named = named_ref[r] > 0
        key = jnp.where(named, order, none)
        least = jnp.min(key, axis=0, keepdims=True)
        least_ref[pl.ds(r, 1), :] = least
        common = jnp.maximum(common, ones(named & (key > least)))
        return common, jnp.maximum(worst, least)

    common, worst = lax.fori_loop(0, n_dev, split_row, (jnp.zeros((per_dev, n_dev), f32), jnp.zeros((1, n_dev), f32)), unroll=8)
    tri = ones(iota((per_dev, per_dev), 0) > iota((per_dev, per_dev), 1))
    rank = dot(tri, common)
    one_row = jnp.ones((8, per_dev), f32)
    source, target = iota((n_dev, n_dev), 0), iota((n_dev, n_dev), 1)
    per_owner = dot(one_row, common)
    same_col = source % n_col == target % n_col
    base = dot(per_owner, ones(same_col & (source < target)))[:1]
    in_all = dot(per_owner, ones(same_col))[:1]
    misfit = jnp.maximum(jnp.max(ones(worst >= none)), jnp.max(ones(in_all > COMMON)))
    in_col = base + rank
    slot = (owner % n_col * COMMON).astype(f32) + in_col
    pick_me = ones(iota((8, n_dev), 1) == me)
    direct = dot(pick_me, (least_ref[...].astype(i32) % per_dev).astype(f32), NT)[:1]
    here = owner == me
    my_common = jnp.sum(jnp.where(here, common, 0.0), axis=1, keepdims=True)
    my_rank = jnp.sum(jnp.where(here, rank, 0.0), axis=1, keepdims=True)
    lane = owner.astype(f32)
    own = jnp.sum(jnp.where((my_common > 0) & (my_rank == lane), local.astype(f32), 0.0), axis=0, keepdims=True)
    in_my_col = (common > 0) & (owner % n_col == me % n_col)
    place_in_z = (owner // n_col * COMMON).astype(f32) + rank
    lane_row = iota((1, n_dev), 1)
    col = jnp.zeros((1, n_dev), f32)
    for k in range(COMMON):
        found = jnp.sum(jnp.where(in_my_col & (in_col == k), place_in_z, 0.0))
        col = jnp.where(lane_row == k, found, col)
    mine = named_ref[me] * common
    before = dot(dot(one_row, mine), ones(source < target))[:1]
    place = jnp.where(mine > 0, dot(tri, mine) + before, -1.0).T
    slot_t = slot.T
    j_lane = target.astype(f32)
    pick = jnp.zeros((n_dev, n_dev), f32)
    for l in range(per_dev):
        pick = pick + jnp.where(place[:, l:l + 1] == j_lane, slot_t[:, l:l + 1], 0.0)
    pick = jnp.sum(pick, axis=0, keepdims=True)
    plan_ref[...] = jnp.zeros(plan_ref.shape, i32)
    for i, value in enumerate((misfit + jnp.zeros((1, n_dev), f32), direct, own, col, pick)):
        plan_ref[i:i + 1, :] = value.astype(i32)


def plan_exchange(block_table):
    n_dev = block_table.shape[0]
    vmem = pl.BlockSpec(memory_space=pltpu.VMEM)
    return pl.pallas_call(
        plan_kernel,
        out_shape=jax.ShapeDtypeStruct((8, n_dev), jnp.int32),
        in_specs=[vmem],
        out_specs=vmem,
        scratch_shapes=[pltpu.VMEM((n_dev, 32, n_dev), jnp.float32), pltpu.VMEM((n_dev, n_dev), jnp.float32)],
        name='plan_exchange')(block_table)


def store_kernel(ids_ref, kp_ref, vp_ref, kn_ref, vn_ref, ko_ref, vo_ref, kv_ref):
    def block(b, carry):
        ko_ref[b] = kp_ref[b]
        vo_ref[b] = vp_ref[b]
        kv_ref[b, 0] = jnp.swapaxes(kp_ref[b], 0, 1)
        kv_ref[b, 1] = jnp.swapaxes(vp_ref[b], 0, 1)
        return carry

    def write(i, carry):
        ko_ref[ids_ref[i]] = kn_ref[i]
        vo_ref[ids_ref[i]] = vn_ref[i]
        return carry

    lax.fori_loop(0, kp_ref.shape[0], block, 0)
    lax.fori_loop(0, kn_ref.shape[0], write, 0)


def store_chunk(k_pool, v_pool, k_new, v_new, write_ids):
    n_blocks, block_len, kv_heads, head_dim = k_pool.shape
    new_shape = (write_ids.size, block_len, kv_heads, head_dim)
    vmem = pl.BlockSpec(memory_space=pltpu.VMEM)
    return pl.pallas_call(
        store_kernel,
        out_shape=(jax.ShapeDtypeStruct(k_pool.shape, k_pool.dtype), jax.ShapeDtypeStruct(v_pool.shape, v_pool.dtype),
                   jax.ShapeDtypeStruct((n_blocks, 2, kv_heads, block_len, head_dim), k_pool.dtype)),
        in_specs=[pl.BlockSpec(memory_space=pltpu.SMEM)] + [vmem] * 4,
        out_specs=(vmem, vmem, vmem),
        name='store_chunk')(write_ids.reshape(-1), k_pool, v_pool, k_new.reshape(new_shape), v_new.reshape(new_shape))


def device_at(z, y, x, c):
    return z * 32 + y * 8 + x * 2 + c


def fused_kernel(plan_ref, q_in, kn_in, vn_in, kv_ref, o_ref,
                 q_ref, kn_ref, vn_ref, zbuf, cbuf, sbuf, wbuf, acc_ref, m_ref, l_ref, s0, s1, s2, s3, p0, p1, p2, p3, f0, f1, f2, f3,
                 z_send, z_recv, a_send, a_recv, b_send, b_recv, c_send, c_recv, w_send, w_recv):
    n_dev, kv_heads = 128, kn_ref.shape[0]
    heads = 4
    q_tile = q_ref.shape[1]
    block_len = kv_ref.shape[3]
    scale = math.log2(math.e) * q_ref.shape[2] ** -0.5
    s_bufs, p_bufs, f_bufs = (s0, s1, s2, s3), (p0, p1, p2, p3), (f0, f1, f2, f3)
    me = lax.axis_index('pool')
    z, y, x, c = me // 32, (me // 8) % 4, (me // 2) % 4, me % 2
    col = me % 32
    other = device_at(z, y, x, 1 - c)
    sign = 1 + 2 * c

    def offset_peer(i):
        r = (i * 11) % 32
        rest = jnp.maximum(i - 32, 0)
        place = rest // 6
        in_plane = jnp.int32(PLACES[-1])
        for n in range(len(PLACES) - 2, -1, -1):
            in_plane = jnp.where(place == n, PLACES[n], in_plane)
        near = i < 32
        in_plane = jnp.where(near, r // 2, in_plane)
        dz = jnp.where(near, 0, rest % 3 + 1)
        dc = jnp.where(near, r, rest % 6 // 3)
        return device_at((z + dz * sign) % 4, (y + in_plane // 4 * sign) % 4, (x + in_plane % 4 * sign) % 4, (c + dc) % 2)

    barrier = pltpu.get_barrier_semaphore()

    def greet(i, carry):
        pl.semaphore_signal(barrier, inc=1, device_id=((me + i) % n_dev,), device_id_type=MESH)
        return carry

    lax.fori_loop(1, n_dev, greet, 0)

    for k in range(COMMON):
        zbuf[z * COMMON + k] = kv_ref[plan_ref[2, k]]

    def fill(i, carry):
        sbuf[i] = kv_ref[plan_ref[1, offset_peer(i)]]
        return carry

    def fill_group(group):
        lax.fori_loop(max(1, group * GROUP), (group + 1) * GROUP, fill, 0)

    fill_group(0)
    wbuf[0] = kv_ref[plan_ref[1, me]]
    pl.semaphore_wait(barrier, n_dev - 1)

    def remote(src, dst, ssem, rsem, peer):
        return pltpu.make_async_remote_copy(src_ref=src, dst_ref=dst, send_sem=ssem, recv_sem=rsem,
                                            device_id=(peer,), device_id_type=MESH)

    z_part = zbuf.at[pl.ds(z * COMMON, COMMON)]
    for s in range(1, 4):
        remote(z_part, z_part, z_send, z_recv, device_at((z + s) % 4, y, x, c)).start()

    def send_direct(group):
        def one(i, carry):
            remote(sbuf.at[i], wbuf.at[i], w_send.at[group], w_recv.at[group], offset_peer(i)).start()
            return carry
        lax.fori_loop(max(1, group * GROUP), (group + 1) * GROUP, one, 0)

    def direct_part(group):
        size = GROUP - 1 if group == 0 else GROUP
        part = wbuf.at[pl.ds(0, size)]
        return remote(part, part, w_send.at[group], w_recv.at[group], other)

    send_direct(0)

    def heads_first(t, carry):
        rows = pl.ds(t * block_len, block_len)
        q_ref[:, rows, :] = jnp.swapaxes(q_in[rows], 0, 1)
        kn_ref[:, rows, :] = jnp.swapaxes(kn_in[rows], 0, 1)
        vn_ref[:, rows, :] = jnp.swapaxes(vn_in[rows], 0, 1)
        return carry

    lax.fori_loop(0, q_tile // block_len, heads_first, 0)

    row = lax.broadcasted_iota(jnp.int32, (kn_ref.shape[1], q_tile), 0)
    token = lax.broadcasted_iota(jnp.int32, (kn_ref.shape[1], q_tile), 1)

    def own_head(g, carry):
        for h in range(heads):
            cols = pl.ds(h * q_tile, q_tile)
            s = lax.dot_general(kn_ref[g], q_ref[g * heads + h], NT, preferred_element_type=jnp.float32)
            s = jnp.where(row <= token, s, -jnp.inf)
            top = jnp.max(s, axis=0, keepdims=True)
            e = jnp.exp2((s - top) * scale)
            m_ref[g, :, cols] = top
            l_ref[g, :, cols] = jnp.sum(e, axis=0, keepdims=True)
            acc_ref[g, :, cols] = lax.dot_general(vn_ref[g], e.astype(jnp.bfloat16), TN, preferred_element_type=jnp.float32)
        return carry

    lax.fori_loop(0, kv_heads, own_head, 0)
    for group in range(1, 4):
        fill_group(group)

    def attend(start):
        def rows_of(which, g):
            return wbuf[pl.ds(start, GROUP), which, g].reshape(GROUP * block_len, kv_ref.shape[4])

        def score(g, h):
            s_bufs[h][...] = lax.dot_general(rows_of(0, g), q_ref[g * heads + h], NT, preferred_element_type=jnp.float32)

        def weigh(g, h):
            cols = pl.ds(h * q_tile, q_tile)
            old = m_ref[g, :, cols]
            top = jnp.maximum(old, jnp.max(s_bufs[h][...], axis=0, keepdims=True))
            fade = jnp.exp2((old - top) * scale)
            e = jnp.exp2((s_bufs[h][...] - top) * scale)
            l_ref[g, :, cols] = l_ref[g, :, cols] * fade + jnp.sum(e, axis=0, keepdims=True)
            p_bufs[h][...] = e.astype(jnp.bfloat16)
            m_ref[g, :, cols] = top
            f_bufs[h][...] = fade

        def add_values(g, h):
            cols = pl.ds(h * q_tile, q_tile)
            part = lax.dot_general(rows_of(1, g), p_bufs[h][...], TN, preferred_element_type=jnp.float32)
            acc_ref[g, :, cols] = acc_ref[g, :, cols] * f_bufs[h][...] + part

        for h in range(heads):
            score(0, h)
        p_bufs[heads - 1][...] = jnp.zeros_like(p_bufs[heads - 1])
        f_bufs[heads - 1][...] = jnp.ones_like(f_bufs[heads - 1])

        def per_group(g, carry):
            following, last = jnp.minimum(g + 1, kv_heads - 1), jnp.maximum(g - 1, 0)
            for h in range(heads):
                if h == 0:
                    add_values(last, heads - 1)
                else:
                    add_values(g, h - 1)
                weigh(g, h)
                score(following, h)
            return carry

        lax.fori_loop(0, kv_heads, per_group, 0)
        add_values(kv_heads - 1, heads - 1)

    y_first = 1 - c

    def line_at(first, second):
        yy = (y + first * y_first + second * (1 - y_first)) % 4
        xx = (x + first * (1 - y_first) + second * y_first) % 4
        return (yy * 8 + xx * 2 + c) * COMMON

    def peer_at(first, second):
        yy = (y + first * y_first + second * (1 - y_first)) % 4
        xx = (x + first * (1 - y_first) + second * y_first) % 4
        return device_at(z, yy, xx, c)

    next_a, prev_a, next_b, prev_b = peer_at(1, 0), peer_at(3, 0), peer_at(0, 1), peer_at(0, 3)
    half = COMMON // 2

    def share(start, size, ssem, rsem, peer):
        part = cbuf.at[pl.ds(start, size)]
        return remote(part, part, ssem, rsem, peer)

    def arrived(blocks, ssem, rsem):
        share(0, blocks, ssem, rsem, other).wait_recv()

    def to_second(i, first):
        start = line_at(first, 0)
        share(start, COMMON, b_send, b_recv.at[3 * i], next_b).start()
        share(start, COMMON, b_send, b_recv.at[3 * i + 1], prev_b).start()
        share(start, COMMON, c_send.at[0], c_recv.at[0], other).start()

    z_three = zbuf.at[pl.ds(0, 3 * COMMON)]
    order = (0, 3, 1, 2)

    remote(z_three, z_three, z_send, z_recv, other).wait_recv()
    for k in range(COMMON):
        cbuf[col * COMMON + k] = zbuf[plan_ref[3, k]]
    share(line_at(0, 0), COMMON, a_send, a_recv.at[0], next_a).start()
    share(line_at(0, 0), COMMON, a_send, a_recv.at[1], prev_a).start()
    to_second(0, 0)
    send_direct(1)
    arrived(COMMON, a_send, a_recv.at[0])
    share(line_at(3, 0), half, a_send, a_recv.at[2], next_a).start()
    to_second(1, 3)
    arrived(COMMON, a_send, a_recv.at[1])
    share(line_at(1, 0) + half, half, a_send, a_recv.at[2], prev_a).start()
    to_second(2, 1)
    arrived(COMMON, a_send, a_recv.at[2])
    to_second(3, 2)
    for i, first in enumerate(order):
        arrived(COMMON, b_send, b_recv.at[3 * i])
        share(line_at(first, 3), half, b_send, b_recv.at[3 * i + 2], next_b).start()
        share(line_at(first, 3), COMMON, c_send.at[1], c_recv.at[1], other).start()
        arrived(COMMON, b_send, b_recv.at[3 * i + 1])
        share(line_at(first, 1) + half, half, b_send, b_recv.at[3 * i + 2], prev_b).start()
        share(line_at(first, 1), COMMON, c_send.at[2], c_recv.at[2], other).start()
    for group in range(2, 4):
        send_direct(group)
    for i, first in enumerate(order):
        arrived(COMMON, b_send, b_recv.at[3 * i + 2])
        share(line_at(first, 2), COMMON, c_send.at[3], c_recv.at[3], other).start()

    def step(t, carry):
        @pl.when(t == 0)
        def _():
            direct_part(0).wait_recv()

        @pl.when(t == 1)
        def _():
            for i in range(4):
                arrived(4 * COMMON, c_send.at[i], c_recv.at[i])

        @pl.when((t >= 1) & (t < 5))
        def _():
            def pick(i, inner):
                wbuf[n_dev + i] = cbuf[plan_ref[4, (t - 1) * GROUP + i]]
                return inner
            lax.fori_loop(0, GROUP, pick, 0)

        for group in range(1, 4):
            @pl.when(t == group + 4)
            def _(group=group):
                direct_part(group).wait_recv()

        attend(jnp.where(t < 1, 0, jnp.where(t < 5, 4, t - 4)) * GROUP)
        return carry

    lax.fori_loop(0, 8, step, 0)

    def finish(g, carry):
        for h in range(heads):
            cols = pl.ds(h * q_tile, q_tile)
            out = acc_ref[g, :, cols] / l_ref[g, :, cols]
            q_ref[g * heads + h] = out.T.astype(jnp.bfloat16)
        return carry

    lax.fori_loop(0, kv_heads, finish, 0)

    def tokens_first(t, carry):
        rows = pl.ds(t * block_len, block_len)
        o_ref[rows] = jnp.swapaxes(q_ref[:, rows, :], 0, 1)
        return carry

    lax.fori_loop(0, q_tile // block_len, tokens_first, 0)
    remote(z_three, z_three, z_send, z_recv, other).wait_send()
    share(0, 3 * COMMON, a_send, a_recv.at[0], other).wait_send()
    share(0, 12 * COMMON, b_send, b_recv.at[0], other).wait_send()
    for i in range(4):
        share(0, 4 * COMMON, c_send.at[i], c_recv.at[i], other).wait_send()
    for group in range(4):
        direct_part(group).wait_send()


def fused_attention(queries, k_new, v_new, kv, plan):
    _, chunk_len, q_heads, head_dim = queries.shape
    kv_heads = k_new.shape[2]
    block = kv.shape[1:]
    q_rows, q_tile = chunk_len * q_heads // kv_heads, chunk_len
    keys = GROUP * block[2]
    bf16, f32 = jnp.bfloat16, jnp.float32
    smem, vmem = pl.BlockSpec(memory_space=pltpu.SMEM), pl.BlockSpec(memory_space=pltpu.VMEM)
    dma = pltpu.SemaphoreType.DMA
    out = pl.pallas_call(
        fused_kernel,
        out_shape=jax.ShapeDtypeStruct(queries.shape[1:], bf16),
        in_specs=[smem] + [vmem] * 4,
        out_specs=vmem,
        scratch_shapes=[
            pltpu.VMEM((q_heads, chunk_len, head_dim), bf16),
            pltpu.VMEM((kv_heads, chunk_len, head_dim), bf16),
            pltpu.VMEM((kv_heads, chunk_len, head_dim), bf16),
            pltpu.VMEM((4 * COMMON,) + block, bf16),
            pltpu.VMEM((32 * COMMON,) + block, bf16),
            pltpu.VMEM((128,) + block, bf16),
            pltpu.VMEM((128 + GROUP,) + block, bf16),
            pltpu.VMEM((kv_heads, head_dim, q_rows), f32),
            pltpu.VMEM((kv_heads, 1, q_rows), f32),
            pltpu.VMEM((kv_heads, 1, q_rows), f32)]
        + [pltpu.VMEM((keys, q_tile), f32)] * 4 + [pltpu.VMEM((keys, q_tile), bf16)] * 4 + [pltpu.VMEM((1, q_tile), f32)] * 4
        + [dma, dma, dma, dma((3,)), dma, dma((12,)), dma((4,)), dma((4,)), dma((4,)), dma((4,))],
        compiler_params=pltpu.CompilerParams(has_side_effects=True, collective_id=0, vmem_limit_bytes=66_000_000),
        name='fused_attention')(plan, queries[0], k_new[0], v_new[0], kv)
    return out


def solution(mesh):
    n_dev = mesh.shape['pool']

    def local_step(queries, k_new, v_new, k_pool, v_pool, block_table, write_ids):
        plan = plan_exchange(block_table)
        k_pool_out, v_pool_out, kv = store_chunk(k_pool, v_pool, k_new, v_new, write_ids)
        attn_out = lax.cond(
            plan[0, 0] == 0,
            lambda: fused_attention(queries, k_new, v_new, kv, plan),
            lambda: general_attention(n_dev, queries, k_new, v_new, k_pool, v_pool, block_table)[0])
        return attn_out[None], k_pool_out, v_pool_out

    row_spec = P('pool')
    return jax.shard_map(local_step, mesh=mesh, in_specs=(row_spec, row_spec, row_spec, row_spec, row_spec, P(), row_spec), out_specs=(row_spec, row_spec, row_spec), check_vma=False)
```

```python
import functools
import math

import jax
import jax.numpy as jnp
from jax import lax
from jax.experimental import pallas as pl
from jax.experimental.pallas import tpu as pltpu
from jax.sharding import PartitionSpec as P

COMMON = 8
GROUP = 32
MESH = pl.DeviceIdType.MESH
PLACES = (0, 1, 3, 4, 12, 5, 15, 2, 8, 7, 13, 6, 9, 14, 11, 10)


def chunk_attention(q_grp, k_pref, v_pref, k_chunk, v_chunk):
    chunk_len = q_grp.shape[1]
    score_scale = q_grp.shape[-1] ** -0.5
    s_pref = jnp.einsum('rcgqd,rtgd->rcgqt', q_grp, k_pref, preferred_element_type=jnp.float32) * score_scale
    s_self = jnp.einsum('rcgqd,rtgd->rcgqt', q_grp, k_chunk, preferred_element_type=jnp.float32) * score_scale
    causal = (jnp.arange(chunk_len)[:, None] >= jnp.arange(chunk_len)[None, :])[None, :, None, None, :]
    s_self = jnp.where(causal, s_self, -jnp.inf)
    row_max = jnp.maximum(jnp.max(s_pref, axis=-1), jnp.max(s_self, axis=-1))[..., None]
    e_pref = jnp.exp(s_pref - row_max)
    e_self = jnp.exp(s_self - row_max)
    prob_total = jnp.sum(e_pref, axis=-1, keepdims=True) + jnp.sum(e_self, axis=-1, keepdims=True)
    p_pref = (e_pref / prob_total).astype(jnp.bfloat16)
    p_self = (e_self / prob_total).astype(jnp.bfloat16)
    attn_acc = jnp.einsum('rcgqt,rtgd->rcgqd', p_pref, v_pref, preferred_element_type=jnp.float32)
    return attn_acc + jnp.einsum('rcgqt,rtgd->rcgqd', p_self, v_chunk, preferred_element_type=jnp.float32)


def general_attention(n_dev, queries, k_new, v_new, k_pool, v_pool, block_table):
    req_count, chunk_len, q_heads, head_dim = queries.shape
    kv_heads = k_new.shape[2]
    per_dev, block_len = k_pool.shape[0], k_pool.shape[1]
    n_pref = block_table.shape[1]
    row_cap = 2 * n_pref // n_dev + (n_pref // 2 + n_dev - 1) // n_dev
    pair_cap = req_count * row_cap
    my_index = lax.axis_index('pool')
    owners = block_table // per_dev
    owned_here = (owners == my_index).reshape(n_dev, req_count * n_pref).astype(jnp.int32)
    send_slot = jnp.where(owned_here > 0, jnp.cumsum(owned_here, axis=1) - 1, pair_cap)
    dest_dev = jnp.broadcast_to(jnp.arange(n_dev)[:, None], send_slot.shape)
    local_ids = (block_table % per_dev).reshape(n_dev, req_count * n_pref)
    send_ids = jnp.zeros((n_dev, pair_cap), jnp.int32).at[dest_dev, send_slot].set(local_ids, mode='drop')
    k_recv = lax.all_to_all(k_pool[send_ids], 'pool', 0, 0, tiled=True)
    v_recv = lax.all_to_all(v_pool[send_ids], 'pool', 0, 0, tiled=True)
    my_owners = lax.dynamic_slice_in_dim(owners, my_index * req_count, req_count, 0).reshape(-1)
    from_owner = (my_owners[:, None] == jnp.arange(n_dev)[None, :]).astype(jnp.int32)
    slot_rank = jnp.sum(from_owner * (jnp.cumsum(from_owner, axis=0) - 1), axis=1)
    recv_idx = (my_owners * pair_cap + slot_rank).reshape(req_count, n_pref)
    flat_shape = (n_dev * pair_cap, block_len, kv_heads, head_dim)
    prefix_shape = (req_count, n_pref * block_len, kv_heads, head_dim)
    k_pref = k_recv.reshape(flat_shape)[recv_idx].reshape(prefix_shape)
    v_pref = v_recv.reshape(flat_shape)[recv_idx].reshape(prefix_shape)
    q_grp = queries.reshape(req_count, chunk_len, kv_heads, q_heads // kv_heads, head_dim)
    attn_acc = chunk_attention(q_grp, k_pref, v_pref, k_new, v_new)
    return attn_acc.reshape(req_count, chunk_len, q_heads, head_dim).astype(jnp.bfloat16)


NT = (((1,), (1,)), ((), ()))
TN = (((0,), (0,)), ((), ()))


def plan_kernel(tab_ref, plan_ref, flag_ref, named_ref, least_ref):
    f32, bf16, i32 = jnp.float32, jnp.bfloat16, jnp.int32
    n_dev, n_pref = tab_ref.shape
    per_dev, n_col = 32, n_dev // 4
    me = lax.axis_index('pool')
    none = 1e6

    def iota(shape, dim):
        return lax.broadcasted_iota(i32, shape, dim)

    def ones(mask):
        return jnp.where(mask, 1.0, 0.0).astype(f32)

    def dot(a, b, dims=(((1,), (0,)), ((), ()))):
        return lax.dot_general(a.astype(bf16), b.astype(bf16), dims, preferred_element_type=f32)

    local_row = iota((per_dev, n_pref), 0)
    owner_row = iota((n_dev, n_pref), 0)
    local = iota((per_dev, n_dev), 0)
    owner = iota((per_dev, n_dev), 1)

    def count_row(r, total):
        row = tab_ref[pl.ds(r, 1), :]
        named = dot(ones(local_row == row % per_dev), ones(owner_row == row // per_dev), NT)
        named_ref[r] = named
        return total + named

    use_count = lax.fori_loop(0, n_dev, count_row, jnp.zeros((per_dev, n_dev), f32), unroll=8)
    order = use_count * per_dev + local.astype(f32)

    def split_row(r, carry):
        common, worst = carry
        named = named_ref[r] > 0
        key = jnp.where(named, order, none)
        least = jnp.min(key, axis=0, keepdims=True)
        least_ref[pl.ds(r, 1), :] = least
        common = jnp.maximum(common, ones(named & (key > least)))
        return common, jnp.maximum(worst, least)

    common, worst = lax.fori_loop(0, n_dev, split_row, (jnp.zeros((per_dev, n_dev), f32), jnp.zeros((1, n_dev), f32)), unroll=8)
    tri = ones(iota((per_dev, per_dev), 0) > iota((per_dev, per_dev), 1))
    rank = dot(tri, common)
    one_row = jnp.ones((8, per_dev), f32)
    source, target = iota((n_dev, n_dev), 0), iota((n_dev, n_dev), 1)
    per_owner = dot(one_row, common)
    same_col = source % n_col == target % n_col
    base = dot(per_owner, ones(same_col & (source < target)))[:1]
    in_all = dot(per_owner, ones(same_col))[:1]
    misfit = jnp.maximum(jnp.max(ones(worst >= none)), jnp.max(ones(in_all > COMMON)))
    in_col = base + rank
    slot = (owner % n_col * COMMON).astype(f32) + in_col
    pick_me = ones(iota((8, n_dev), 1) == me)
    direct = dot(pick_me, (least_ref[...].astype(i32) % per_dev).astype(f32), NT)[:1]
    here = owner == me
    my_common = jnp.sum(jnp.where(here, common, 0.0), axis=1, keepdims=True)
    my_rank = jnp.sum(jnp.where(here, rank, 0.0), axis=1, keepdims=True)
    lane = owner.astype(f32)
    own = jnp.sum(jnp.where((my_common > 0) & (my_rank == lane), local.astype(f32), 0.0), axis=0, keepdims=True)
    in_my_col = (common > 0) & (owner % n_col == me % n_col)
    place_in_z = (owner // n_col * COMMON).astype(f32) + rank
    lane_row = iota((1, n_dev), 1)
    col = jnp.zeros((1, n_dev), f32)
    for k in range(COMMON):
        found = jnp.sum(jnp.where(in_my_col & (in_col == k), place_in_z, 0.0))
        col = jnp.where(lane_row == k, found, col)
    mine = named_ref[me] * common
    before = dot(dot(one_row, mine), ones(source < target))[:1]
    place = jnp.where(mine > 0, dot(tri, mine) + before, -1.0).T
    slot_t = slot.T
    j_lane = target.astype(f32)
    pick = jnp.zeros((n_dev, n_dev), f32)
    for l in range(per_dev):
        pick = pick + jnp.where(place[:, l:l + 1] == j_lane, slot_t[:, l:l + 1], 0.0)
    pick = jnp.sum(pick, axis=0, keepdims=True)
    flag_ref[0] = misfit.astype(i32)
    plan_ref[...] = jnp.zeros(plan_ref.shape, i32)
    for i, value in enumerate((misfit + jnp.zeros((1, n_dev), f32), direct, own, col, pick)):
        plan_ref[i:i + 1, :] = value.astype(i32)


def plan_exchange(block_table):
    n_dev = block_table.shape[0]
    vmem = pl.BlockSpec(memory_space=pltpu.VMEM)
    return pl.pallas_call(
        plan_kernel,
        out_shape=(jax.ShapeDtypeStruct((8, n_dev), jnp.int32), jax.ShapeDtypeStruct((1,), jnp.int32)),
        in_specs=[vmem],
        out_specs=(vmem, pl.BlockSpec(memory_space=pltpu.SMEM)),
        scratch_shapes=[pltpu.VMEM((n_dev, 32, n_dev), jnp.float32), pltpu.VMEM((n_dev, n_dev), jnp.float32)],
        name='plan_exchange')(block_table)


def store_kernel(ids_ref, kp_ref, vp_ref, kn_ref, vn_ref, ko_ref, vo_ref, kv_ref):
    def block(b, carry):
        ko_ref[b] = kp_ref[b]
        vo_ref[b] = vp_ref[b]
        kv_ref[b, 0] = jnp.swapaxes(kp_ref[b], 0, 1)
        kv_ref[b, 1] = jnp.swapaxes(vp_ref[b], 0, 1)
        return carry

    def write(i, carry):
        ko_ref[ids_ref[i]] = kn_ref[i]
        vo_ref[ids_ref[i]] = vn_ref[i]
        return carry

    lax.fori_loop(0, kp_ref.shape[0], block, 0)
    lax.fori_loop(0, kn_ref.shape[0], write, 0)


def store_chunk(k_pool, v_pool, k_new, v_new, write_ids):
    n_blocks, block_len, kv_heads, head_dim = k_pool.shape
    new_shape = (write_ids.size, block_len, kv_heads, head_dim)
    vmem = pl.BlockSpec(memory_space=pltpu.VMEM)
    return pl.pallas_call(
        store_kernel,
        out_shape=(jax.ShapeDtypeStruct(k_pool.shape, k_pool.dtype), jax.ShapeDtypeStruct(v_pool.shape, v_pool.dtype),
                   jax.ShapeDtypeStruct((n_blocks, 2, kv_heads, block_len, head_dim), k_pool.dtype)),
        in_specs=[pl.BlockSpec(memory_space=pltpu.SMEM)] + [vmem] * 4,
        out_specs=(vmem, vmem, vmem),
        name='store_chunk')(write_ids.reshape(-1), k_pool, v_pool, k_new.reshape(new_shape), v_new.reshape(new_shape))


def device_at(z, y, x, c):
    return z * 32 + y * 8 + x * 2 + c


def fused_kernel(plan_ref, q_in, kn_in, vn_in, kv_ref, o_ref,
                 q_ref, kn_ref, vn_ref, zbuf, cbuf, sbuf, wbuf, acc_ref, m_ref, l_ref, s0, s1, s2, s3, p0, p1, p2, p3, f0, f1, f2, f3,
                 z_send, z_recv, a_send, a_recv, b_send, b_recv, c_send, c_recv, w_send, w_recv):
    n_dev, kv_heads = 128, kn_ref.shape[0]
    heads = 4
    q_tile = q_ref.shape[1]
    block_len = kv_ref.shape[3]
    scale = math.log2(math.e) * q_ref.shape[2] ** -0.5
    s_bufs, p_bufs, f_bufs = (s0, s1, s2, s3), (p0, p1, p2, p3), (f0, f1, f2, f3)
    me = lax.axis_index('pool')
    z, y, x, c = me // 32, (me // 8) % 4, (me // 2) % 4, me % 2
    col = me % 32
    other = device_at(z, y, x, 1 - c)
    sign = 1 + 2 * c

    def offset_peer(i):
        r = (i * 11) % 32
        rest = jnp.maximum(i - 32, 0)
        place = rest // 6
        in_plane = jnp.int32(PLACES[-1])
        for n in range(len(PLACES) - 2, -1, -1):
            in_plane = jnp.where(place == n, PLACES[n], in_plane)
        near = i < 32
        in_plane = jnp.where(near, r // 2, in_plane)
        dz = jnp.where(near, 0, rest % 3 + 1)
        dc = jnp.where(near, r, rest % 6 // 3)
        return device_at((z + dz * sign) % 4, (y + in_plane // 4 * sign) % 4, (x + in_plane % 4 * sign) % 4, (c + dc) % 2)

    groups = n_dev // GROUP
    near_groups = groups // 4
    barrier = pltpu.get_barrier_semaphore()

    def greet(i, carry):
        pl.semaphore_signal(barrier, inc=1, device_id=((me + i) % n_dev,), device_id_type=MESH)
        return carry

    lax.fori_loop(1, n_dev, greet, 0)

    for k in range(COMMON):
        zbuf[z * COMMON + k] = kv_ref[plan_ref[2, k]]

    def fill(i, carry):
        sbuf[i] = kv_ref[plan_ref[1, offset_peer(i)]]
        return carry

    def fill_group(group):
        lax.fori_loop(max(1, group * GROUP), (group + 1) * GROUP, fill, 0)

    for group in range(near_groups):
        fill_group(group)
    wbuf[0] = kv_ref[plan_ref[1, me]]
    pl.semaphore_wait(barrier, n_dev - 1)

    def remote(src, dst, ssem, rsem, peer):
        return pltpu.make_async_remote_copy(src_ref=src, dst_ref=dst, send_sem=ssem, recv_sem=rsem,
                                            device_id=(peer,), device_id_type=MESH)

    z_part = zbuf.at[pl.ds(z * COMMON, COMMON)]
    for s in range(1, 4):
        remote(z_part, z_part, z_send, z_recv, device_at((z + s) % 4, y, x, c)).start()

    def send_direct(group):
        def one(i, carry):
            remote(sbuf.at[i], wbuf.at[i], w_send.at[group], w_recv.at[group], offset_peer(i)).start()
            return carry
        lax.fori_loop(max(1, group * GROUP), (group + 1) * GROUP, one, 0)

    def direct_part(group):
        size = GROUP - 1 if group == 0 else GROUP
        part = wbuf.at[pl.ds(0, size)]
        return remote(part, part, w_send.at[group], w_recv.at[group], other)

    for group in range(near_groups):
        send_direct(group)

    def heads_first(t, carry):
        rows = pl.ds(t * block_len, block_len)
        q_ref[:, rows, :] = jnp.swapaxes(q_in[rows], 0, 1)
        kn_ref[:, rows, :] = jnp.swapaxes(kn_in[rows], 0, 1)
        vn_ref[:, rows, :] = jnp.swapaxes(vn_in[rows], 0, 1)
        return carry

    lax.fori_loop(0, q_tile // block_len, heads_first, 0)

    row = lax.broadcasted_iota(jnp.int32, (kn_ref.shape[1], q_tile), 0)
    token = lax.broadcasted_iota(jnp.int32, (kn_ref.shape[1], q_tile), 1)

    def own_head(g, carry):
        for h in range(heads):
            cols = pl.ds(h * q_tile, q_tile)
            s = lax.dot_general(kn_ref[g], q_ref[g * heads + h], NT, preferred_element_type=jnp.float32)
            s = jnp.where(row <= token, s, -jnp.inf)
            top = jnp.max(s, axis=0, keepdims=True)
            e = jnp.exp2((s - top) * scale)
            m_ref[g, :, cols] = top
            l_ref[g, :, cols] = jnp.sum(e, axis=0, keepdims=True)
            acc_ref[g, :, cols] = lax.dot_general(vn_ref[g], e.astype(jnp.bfloat16), TN, preferred_element_type=jnp.float32)
        return carry

    lax.fori_loop(0, kv_heads, own_head, 0)
    for group in range(near_groups, groups):
        fill_group(group)

    def attend(start):
        def rows_of(which, g):
            return wbuf[pl.ds(start, GROUP), which, g].reshape(GROUP * block_len, kv_ref.shape[4])

        def score(g, h):
            s_bufs[h][...] = lax.dot_general(rows_of(0, g), q_ref[g * heads + h], NT, preferred_element_type=jnp.float32)

        def weigh(g, h):
            cols = pl.ds(h * q_tile, q_tile)
            old = m_ref[g, :, cols]
            top = jnp.maximum(old, jnp.max(s_bufs[h][...], axis=0, keepdims=True))
            fade = jnp.exp2((old - top) * scale)
            e = jnp.exp2((s_bufs[h][...] - top) * scale)
            l_ref[g, :, cols] = l_ref[g, :, cols] * fade + jnp.sum(e, axis=0, keepdims=True)
            p_bufs[h][...] = e.astype(jnp.bfloat16)
            m_ref[g, :, cols] = top
            f_bufs[h][...] = fade

        def add_values(g, h):
            cols = pl.ds(h * q_tile, q_tile)
            part = lax.dot_general(rows_of(1, g), p_bufs[h][...], TN, preferred_element_type=jnp.float32)
            acc_ref[g, :, cols] = acc_ref[g, :, cols] * f_bufs[h][...] + part

        for h in range(heads):
            score(0, h)
        p_bufs[heads - 1][...] = jnp.zeros_like(p_bufs[heads - 1])
        f_bufs[heads - 1][...] = jnp.ones_like(f_bufs[heads - 1])

        def per_group(g, carry):
            following, last = jnp.minimum(g + 1, kv_heads - 1), jnp.maximum(g - 1, 0)
            for h in range(heads):
                if h == 0:
                    add_values(last, heads - 1)
                else:
                    add_values(g, h - 1)
                weigh(g, h)
                score(following, h)
            return carry

        lax.fori_loop(0, kv_heads, per_group, 0)
        add_values(kv_heads - 1, heads - 1)

    y_first = 1 - c

    def line_at(first, second):
        yy = (y + first * y_first + second * (1 - y_first)) % 4
        xx = (x + first * (1 - y_first) + second * y_first) % 4
        return (yy * 8 + xx * 2 + c) * COMMON

    def peer_at(first, second):
        yy = (y + first * y_first + second * (1 - y_first)) % 4
        xx = (x + first * (1 - y_first) + second * y_first) % 4
        return device_at(z, yy, xx, c)

    next_a, prev_a, next_b, prev_b = peer_at(1, 0), peer_at(3, 0), peer_at(0, 1), peer_at(0, 3)
    half = COMMON // 2

    def share(start, size, ssem, rsem, peer):
        part = cbuf.at[pl.ds(start, size)]
        return remote(part, part, ssem, rsem, peer)

    def arrived(blocks, ssem, rsem):
        share(0, blocks, ssem, rsem, other).wait_recv()

    def to_second(i, first):
        start = line_at(first, 0)
        share(start, COMMON, b_send, b_recv.at[3 * i], next_b).start()
        share(start, COMMON, b_send, b_recv.at[3 * i + 1], prev_b).start()
        share(start, COMMON, c_send.at[0], c_recv.at[0], other).start()

    z_three = zbuf.at[pl.ds(0, 3 * COMMON)]
    order = (0, 3, 1, 2)

    remote(z_three, z_three, z_send, z_recv, other).wait_recv()
    for k in range(COMMON):
        cbuf[col * COMMON + k] = zbuf[plan_ref[3, k]]
    share(line_at(0, 0), COMMON, a_send, a_recv.at[0], next_a).start()
    share(line_at(0, 0), COMMON, a_send, a_recv.at[1], prev_a).start()
    to_second(0, 0)
    for group in range(near_groups, 2 * near_groups):
        send_direct(group)
    arrived(COMMON, a_send, a_recv.at[0])
    share(line_at(3, 0), half, a_send, a_recv.at[2], next_a).start()
    to_second(1, 3)
    arrived(COMMON, a_send, a_recv.at[1])
    share(line_at(1, 0) + half, half, a_send, a_recv.at[2], prev_a).start()
    to_second(2, 1)
    arrived(COMMON, a_send, a_recv.at[2])
    to_second(3, 2)
    for i, first in enumerate(order):
        arrived(COMMON, b_send, b_recv.at[3 * i])
        share(line_at(first, 3), half, b_send, b_recv.at[3 * i + 2], next_b).start()
        share(line_at(first, 3), COMMON, c_send.at[1], c_recv.at[1], other).start()
        arrived(COMMON, b_send, b_recv.at[3 * i + 1])
        share(line_at(first, 1) + half, half, b_send, b_recv.at[3 * i + 2], prev_b).start()
        share(line_at(first, 1), COMMON, c_send.at[2], c_recv.at[2], other).start()
    for group in range(2 * near_groups, groups):
        send_direct(group)
    for i, first in enumerate(order):
        arrived(COMMON, b_send, b_recv.at[3 * i + 2])
        share(line_at(first, 2), COMMON, c_send.at[3], c_recv.at[3], other).start()

    last_common = near_groups + groups

    def step(t, carry):
        for group in range(groups):
            @pl.when(t == (group if group < near_groups else group + groups))
            def _(group=group):
                direct_part(group).wait_recv()

        @pl.when(t == near_groups)
        def _():
            for i in range(4):
                arrived(4 * COMMON, c_send.at[i], c_recv.at[i])

        @pl.when((t >= near_groups) & (t < last_common))
        def _():
            def pick(i, inner):
                wbuf[n_dev + i] = cbuf[plan_ref[4, (t - near_groups) * GROUP + i]]
                return inner
            lax.fori_loop(0, GROUP, pick, 0)

        attend(jnp.where(t < near_groups, t, jnp.where(t < last_common, groups, t - groups)) * GROUP)
        return carry

    lax.fori_loop(0, 2 * groups, step, 0)

    def finish(g, carry):
        for h in range(heads):
            cols = pl.ds(h * q_tile, q_tile)
            out = acc_ref[g, :, cols] / l_ref[g, :, cols]
            q_ref[g * heads + h] = out.T.astype(jnp.bfloat16)
        return carry

    lax.fori_loop(0, kv_heads, finish, 0)

    def tokens_first(t, carry):
        rows = pl.ds(t * block_len, block_len)
        o_ref[rows] = jnp.swapaxes(q_ref[:, rows, :], 0, 1)
        return carry

    lax.fori_loop(0, q_tile // block_len, tokens_first, 0)
    remote(z_three, z_three, z_send, z_recv, other).wait_send()
    share(0, 3 * COMMON, a_send, a_recv.at[0], other).wait_send()
    share(0, 12 * COMMON, b_send, b_recv.at[0], other).wait_send()
    for i in range(4):
        share(0, 4 * COMMON, c_send.at[i], c_recv.at[i], other).wait_send()
    for group in range(groups):
        direct_part(group).wait_send()


def fused_attention(queries, k_new, v_new, kv, plan):
    _, chunk_len, q_heads, head_dim = queries.shape
    kv_heads = k_new.shape[2]
    block = kv.shape[1:]
    q_rows, q_tile = chunk_len * q_heads // kv_heads, chunk_len
    keys = GROUP * block[2]
    bf16, f32 = jnp.bfloat16, jnp.float32
    smem, vmem = pl.BlockSpec(memory_space=pltpu.SMEM), pl.BlockSpec(memory_space=pltpu.VMEM)
    dma = pltpu.SemaphoreType.DMA
    out = pl.pallas_call(
        fused_kernel,
        out_shape=jax.ShapeDtypeStruct(queries.shape[1:], bf16),
        in_specs=[smem] + [vmem] * 4,
        out_specs=vmem,
        scratch_shapes=[
            pltpu.VMEM((q_heads, chunk_len, head_dim), bf16),
            pltpu.VMEM((kv_heads, chunk_len, head_dim), bf16),
            pltpu.VMEM((kv_heads, chunk_len, head_dim), bf16),
            pltpu.VMEM((4 * COMMON,) + block, bf16),
            pltpu.VMEM((32 * COMMON,) + block, bf16),
            pltpu.VMEM((128,) + block, bf16),
            pltpu.VMEM((128 + GROUP,) + block, bf16),
            pltpu.VMEM((kv_heads, head_dim, q_rows), f32),
            pltpu.VMEM((kv_heads, 1, q_rows), f32),
            pltpu.VMEM((kv_heads, 1, q_rows), f32)]
        + [pltpu.VMEM((keys, q_tile), f32)] * 4 + [pltpu.VMEM((keys, q_tile), bf16)] * 4 + [pltpu.VMEM((1, q_tile), f32)] * 4
        + [dma, dma, dma, dma((3,)), dma, dma((12,)), dma((4,)), dma((4,)), dma((128 // GROUP,)), dma((128 // GROUP,))],
        compiler_params=pltpu.CompilerParams(has_side_effects=True, collective_id=0, vmem_limit_bytes=66_000_000),
        name='fused_attention')(plan, queries[0], k_new[0], v_new[0], kv)
    return out


def solution(mesh):
    n_dev = mesh.shape['pool']

    def local_step(queries, k_new, v_new, k_pool, v_pool, block_table, write_ids):
        plan, misfit = plan_exchange(block_table)
        k_pool_out, v_pool_out, kv = store_chunk(k_pool, v_pool, k_new, v_new, write_ids)
        attn_out = lax.cond(
            misfit[0] == 0,
            lambda: fused_attention(queries, k_new, v_new, kv, plan),
            lambda: general_attention(n_dev, queries, k_new, v_new, k_pool, v_pool, block_table)[0])
        return attn_out[None], k_pool_out, v_pool_out

    row_spec = P('pool')
    return jax.shard_map(local_step, mesh=mesh, in_specs=(row_spec, row_spec, row_spec, row_spec, row_spec, P(), row_spec), out_specs=(row_spec, row_spec, row_spec), check_vma=False)
```
